32 devices in a mesh: row: 2 (over core), col: 4 (over y, x), depth: 4 (over z).
Axes of the slice: x: 2, y: 2, z: 4, core: 2. Of those that a mesh axis runs over, the one named last changes fastest.
Arguments:
- a_tile: float32 [2048, 2048], P('row', 'col'), as said below
- panels: float32 [2048, 4096], P('row', 'depth'), as said below
Outputs:
- trailing: float32 [2048, 2048], P(('row', 'depth'), 'col')
- new_panel: float32 [2048, 512], P(('row', 'col'))
- diag_norm: float32 [1], replicated
Inputs may be any that keep to these rules, and one draw needn't show every extreme that they name: symmetric; a_tile - panels panels^T is positive definite with a large positive diagonal. `panels`: real-valued entries of full rank.
All inputs are finite; a program needn't handle non-finite values.
Results may differ from the reference program's by a relative error of at most 0.00015.
Values sent between devices are 32-bit elements; how exact they have to be, the bound alone decides.
A program may use at most 64 MiB of HBM per device.

```python
import jax
import jax.numpy as jnp
from jax import lax

PB = 512
M = 2048
KTOT = 4096


def panel_matrix(key):
    key_panel = jax.random.fold_in(key, 21)
    deviation = jnp.sqrt(1.5 / jnp.sqrt(jnp.float32(M) * jnp.float32(KTOT)))
    base = jnp.clip(jax.random.normal(key_panel, (M, KTOT), jnp.float32), -6.0, 6.0)
    return (base * deviation).astype(jnp.float32)


def draw_panels(key, part):
    return panel_matrix(key)


def draw_a_tile(key, part):
    key_noise = jax.random.fold_in(key, 11)
    key_diag = jax.random.fold_in(key, 12)
    noise = jax.random.normal(key_noise, (M, M), jnp.float32)
    spread = jax.random.uniform(key_diag, (M,), jnp.float32, 1.0, 1.5)
    noise = noise * (0.5 / jnp.sqrt(jnp.float32(M)))
    symmetric = (noise + noise.T) * 0.7071
    rising = jnp.power(3.0, jnp.arange(M, dtype=jnp.float32) / M)
    diagonal = 4.0 * rising * spread
    panel_full = panel_matrix(key)
    product = jnp.dot(panel_full, panel_full.T, precision=lax.Precision.HIGHEST, preferred_element_type=jnp.float32)
    product = (product + product.T) * 0.5
    return (symmetric + jnp.diag(diagonal) + product).astype(jnp.float32)


def setup_inputs(seed: int = 0) -> dict:
    splits = jax.random.split(jax.random.key(seed), 3)
    a_tile = draw_a_tile(jax.random.fold_in(splits[2], 71), 0)
    panels = draw_panels(jax.random.fold_in(splits[2], 71), 0)
    return dict(a_tile=a_tile, panels=panels)


def reference(a_tile, panels):
    product = jnp.dot(panels.astype(jnp.float32), panels.T.astype(jnp.float32), precision=lax.Precision.HIGHEST, preferred_element_type=jnp.float32)
    trailing = a_tile - product
    factor = jnp.linalg.cholesky(trailing[:PB, :PB])
    new_panel = jax.scipy.linalg.solve_triangular(factor, trailing[:, :PB].T, lower=True).T
    diagonal = jnp.diagonal(trailing)
    diag_norm = jnp.sqrt(jnp.sum(diagonal * diagonal) / M).reshape(1)
    return (trailing, new_panel, diag_norm)
```

```python
import functools

import jax
import jax.numpy as jnp
from jax import lax
from jax.experimental import pallas as pl
from jax.experimental.pallas import tpu as pltpu
from jax.sharding import PartitionSpec as P

PB = 512
BLOCK = 128
NB = 32
LANES = 128
TILE = 256
EVENTS = {"open": 20.0, "tick": 1.15, "first": 13.0, "step": 2.8, "hop": 4.5}
HIGHEST = lax.Precision.HIGHEST
MESH = pl.DeviceIdType.MESH
F32 = jnp.float32
BF16 = jnp.bfloat16


def split(value):
    high = value.astype(BF16)
    return high, (value - high.astype(F32)).astype(BF16)


def dot_t(left, right):
    return lax.dot_general(left, right, (((1,), (1,)), ((), ())), preferred_element_type=F32)


def product(left_hi, left_lo, right_hi, right_lo):
    return dot_t(left_hi, right_hi) + (dot_t(left_hi, right_lo) + dot_t(left_lo, right_hi))


def mm(a, b, dims):
    return lax.dot_general(a, b, (dims, ((), ())), precision=HIGHEST, preferred_element_type=F32)


def factor_block(work, block, advance):
    work[:, :BLOCK] = block
    diag = lax.broadcasted_iota(jnp.int32, (BLOCK, BLOCK), 0) == lax.broadcasted_iota(jnp.int32, (BLOCK, BLOCK), 1)
    work[:, BLOCK:] = jnp.where(diag, 1.0, 0.0)
    sub = lax.broadcasted_iota(jnp.int32, (NB, BLOCK), 0)
    for j in range(0, BLOCK, NB):
        left = work[j:j + NB, :BLOCK]
        right = work[j:j + NB, BLOCK:]
        advance()
        lanes = [jnp.broadcast_to(left[:, j + k:j + k + 1], (NB, BLOCK)) for k in range(NB)]
        for k in range(NB):
            inv = lax.rsqrt(lanes[k][k:k + 1])
            col = lanes[k] * inv
            for i in range(k + 1, NB):
                lanes[i] = lanes[i] - col * col[i:i + 1]
            row_l = left[k:k + 1] * inv
            row_r = right[k:k + 1] * inv
            below = jnp.where(sub > k, col, 0.0)
            left = jnp.where(sub == k, row_l, left - below * row_l)
            right = jnp.where(sub == k, row_r, right - below * row_r)
        work[j:j + NB, :BLOCK] = left
        work[j:j + NB, BLOCK:] = right
        if j + NB < BLOCK:
            both = jnp.concatenate([left, right], axis=1)
            work[j + NB:, :] = work[j + NB:, :] - mm(left[:, j + NB:], both, ((0,), (0,)))
    return work[:, BLOCK:]


def plan(nr, nc, heads):
    lists = [[] for _ in range(nr * nc)]
    for g in range(heads, nr * nc):
        lists[g] = [(g, j) for j in range(heads)] + [(g, g)]
    for low in range(heads, nr * nc):
        for high in range(low + 1, nr * nc):
            able = [g for g in range(nr * nc) if g < nc or g // nc == low // nc]
            best = min(able, key=lambda g: (len(lists[g]), g not in (low, high), g))
            lists[best].append((low, high) if best == low else (high, low))
    return lists


def kernel(sizes, lists, a_ref, p_ref, out_ref, x_ref, n_ref, *scratch):
    nr, nc, nd = sizes
    (hi, lo, oth, part, rin, fin, turned, tin, dpart, drin, d_ref, adbuf, acbuf, psum, nbuf,
     work, invs, fact, rest,
     pair_send, pair_recv, ad_send, ad_recv, ac_send, ac_recv, in_send, in_recv, out_send, out_recv,
     di_send, di_recv, do_send, do_recv, d_send, d_recv, f_send, f_recv, t_send, t_recv, n_send, n_recv) = scratch
    tile_rows, tile_cols = a_ref.shape
    size = tile_rows // nc
    half = size // 2
    heads = PB // size
    wide = tile_cols // size
    share = tile_rows // nd
    sub = BLOCK // nc
    steps = PB // BLOCK
    slots = max(map(len, lists))
    devices = nr * nc * nd
    r, c, z = lax.axis_index("row"), lax.axis_index("col"), lax.axis_index("depth")
    g = r * nc + c
    mid = nd // 2
    low = z < mid
    center = jnp.logical_or(z == mid - 1, z == mid)
    edge = jnp.logical_or(z == 0, z == nd - 1)
    inner = jnp.logical_not(edge)
    side = jnp.where(center, 1, 0)
    inward = jnp.where(low, z + 1, z - 1)
    outward = jnp.where(low, z - 1, z + 1)
    zb = z * share // size
    zo = lax.rem(z * share, size)
    first, second = r == 0, r != 0
    partner = (1 - r, c, z)
    both = jnp.logical_and

    def pick(values):
        result = jnp.int32(values[0])
        for i, value in enumerate(values[1:], 1):
            result = jnp.where(g == i, value, result)
        return result

    xs = [pick([l[s][0] if s < len(l) else 0 for l in lists]) for s in range(slots)]
    ys = [pick([l[s][1] if s < len(l) else 0 for l in lists]) for s in range(slots)]
    counts = pick([len(l) for l in lists])
    valid = [s < counts for s in range(slots)]
    near = [both(valid[s], both(xs[s] // nc == r, ys[s] // nc == r)) for s in range(slots)]
    far = [both(valid[s], jnp.logical_not(both(xs[s] // nc == r, ys[s] // nc == r))) for s in range(slots)]

    def remote(src, dst, send, recv, device):
        return pltpu.make_async_remote_copy(
            src_ref=src, dst_ref=dst, send_sem=send, recv_sem=recv, device_id=device, device_id_type=MESH)

    def rows(start, count):
        return pl.ds(pl.multiple_of(start, count), count)

    barrier = pltpu.get_barrier_semaphore()
    me = g * nd + z

    def device(i):
        there = lax.rem(me + i, devices)
        return (there // (nc * nd), lax.rem(there // nd, nc), lax.rem(there, nd))

    @pl.loop(1, devices)
    def _(i):
        pl.semaphore_signal(barrier, inc=1, device_id=device(i), device_id_type=MESH)

    @pl.loop(0, tile_rows // TILE)
    def _(t):
        high, rem = split(p_ref[rows(t * TILE, TILE), :])
        here = rows(r * tile_rows + t * TILE, TILE)
        hi[here, :] = high
        lo[here, :] = rem

    def compute(s):
        a, b = rows(xs[s] * size, size), rows(ys[s] * size, size)
        part[s] = -product(hi[a, :], lo[a, :], hi[b, :], lo[b, :])

    @pl.when(first)
    def _():
        at = [pl.ds(pl.multiple_of(k * BLOCK + c * sub, sub), sub) for k in range(steps)]
        left_hi = jnp.concatenate([hi[i, :] for i in at], axis=0)
        left_lo = jnp.concatenate([lo[i, :] for i in at], axis=0)
        dpart[...] = -product(left_hi, left_lo, hi[:PB, :], lo[:PB, :])

    for s in range(slots):
        pl.when(near[s])(functools.partial(compute, s))

    pl.semaphore_wait(barrier, devices - 1)

    def pair_copy(j):
        return remote(p_ref.at[rows(j * size, size), :], oth.at[j], pair_send.at[j], pair_recv.at[j], partner)

    def d_fold(k):
        return mid - 1 + k % 2

    def c_fold(q):
        return (mid - 1, mid, 0, nd - 1)[q % 4]

    def d_at(col, k):
        return (pl.ds(pl.multiple_of(k * BLOCK + col * sub, sub), sub), pl.ds(k * BLOCK, PB - k * BLOCK))

    def d_in(k):
        return (pl.ds(k * sub, sub), pl.ds(k * BLOCK, PB - k * BLOCK))

    def ad_copy(k, to):
        return remote(a_ref.at[d_at(to, k)], adbuf.at[d_in(k)], ad_send.at[k, to], ad_recv.at[k], (r, to, z))

    def ac_at(col, q):
        return (rows(col * size + q % 2 * half, half), pl.ds(q // 2 * size, size))

    def ac_copy(q, to):
        return remote(a_ref.at[ac_at(to, q)], acbuf.at[q], ac_send.at[q, to], ac_recv.at[q], (r, to, z))

    @pl.when(first)
    def _():
        for j in range(heads):
            pair_copy(j).start()

    @pl.when(second)
    def _():
        for j in range(nc):
            pair_copy(j).start()

    def folds(act):
        @pl.when(c == 0)
        def _():
            for k in range(steps):
                @pl.when(both(first, z == d_fold(k)))
                def _():
                    for to in range(1, nc):
                        act(ad_copy(k, to))
            for q in range(2 * heads):
                for to in range(1, nc):
                    @pl.when(both(z == c_fold(q), r * nc + to >= heads))
                    def _():
                        act(ac_copy(q, to))

    folds(lambda copy: copy.start())

    def din_copy(k):
        return remote(dpart.at[d_in(k)], drin.at[(side,) + d_in(k)], di_send.at[k], di_recv.at[side, k], (r, c, inward))

    def din_wait(at, k):
        here = drin.at[(at,) + d_in(k)]
        remote(here, here, di_send.at[k], di_recv.at[at, k], (r, c, inward)).wait_recv()
        return here

    def stage_d(k):
        @pl.when(inner)
        def _():
            dpart[d_in(k)] = dpart[d_in(k)] + din_wait(0, k)[...]

        @pl.when(z == d_fold(k))
        def _():
            @pl.when(c == 0)
            def _():
                dpart[d_in(k)] = dpart[d_in(k)] + a_ref[d_at(0, k)]

            @pl.when(c != 0)
            def _():
                ad_copy(k, 1).wait_recv()
                dpart[d_in(k)] = dpart[d_in(k)] + adbuf[d_in(k)]

        din_copy(k).start()

    def dout_copy(k):
        here = d_ref.at[d_at(c, k)]
        return remote(here, here, do_send.at[k], do_recv.at[k], (r, c, outward))

    def d_copy(k, m):
        here = d_ref.at[d_at(c, k)]
        return remote(here, here, d_send.at[k, m], d_recv.at[k, m], (r, lax.rem(c + m, nc), z))

    def d_from(k, m):
        there = d_ref.at[d_at(lax.rem(c - m + nc, nc), k)]
        return remote(there, there, d_send.at[k, m], d_recv.at[k, m], (r, lax.rem(c + m, nc), z))

    def f_copy(k, m):
        there = d_ref.at[d_at(lax.rem(c - m + nc, nc), k)]
        return remote(there, there, f_send.at[k, m], f_recv.at[k, m], partner)

    def spread_d(k):
        @pl.when(inner)
        def _():
            dout_copy(k).start()

        for m in range(1, nc):
            d_copy(k, m).start()
        f_copy(k, 0).start()

    def chunk(q):
        return (q // 2, pl.ds(q % 2 * half, half), slice(None))

    def in_copy(q):
        return remote(part.at[chunk(q)], rin.at[(side,) + chunk(q)], in_send.at[q], in_recv.at[side, q], (r, c, inward))

    def in_wait(at, q):
        here = rin.at[(at,) + chunk(q)]
        remote(here, here, in_send.at[q], in_recv.at[at, q], (r, c, inward)).wait_recv()
        return here

    def out_copy(q):
        here = fin.at[chunk(q)]
        return remote(here, here, out_send.at[q], out_recv.at[q], (r, c, outward))

    def stage_a(q):
        @pl.when(inner)
        def _():
            part[chunk(q)] = part[chunk(q)] + in_wait(0, q)[...]

        if q < 2 * heads:
            @pl.when(both(g >= heads, z == c_fold(q)))
            def _():
                @pl.when(c == 0)
                def _():
                    part[chunk(q)] = part[chunk(q)] + a_ref[ac_at(0, q)]

                @pl.when(c != 0)
                def _():
                    ac_copy(q, 1).wait_recv()
                    part[chunk(q)] = part[chunk(q)] + acbuf[q]

        in_copy(q).start()

    def here_is(device):
        return both(device[0] == r, device[1] == c)

    def routes(s):
        x, y = xs[s], ys[s]
        straight = (x // nc, y // wide, z)
        across = (y // nc, x // wide, z)
        return (
            (both(valid[s], zb == lax.rem(x, nc)), fin.at[s, rows(zo, share), :], lax.rem(y, wide), straight),
            (both(both(valid[s], x != y), zb == lax.rem(y, nc)), turned.at[s, rows(zo, share), :], lax.rem(x, wide), across),
        )

    def deliver(s):
        for way, (cond, src, spot, to) in enumerate(routes(s)):
            @pl.when(cond)
            def _():
                if way:
                    turned[s] = fin[s].T

                @pl.when(here_is(to))
                def _():
                    pltpu.make_async_copy(src, tin.at[spot], t_recv.at[spot]).start()

                @pl.when(jnp.logical_not(here_is(to)))
                def _():
                    remote(src, tin.at[spot], t_send.at[s, way], t_recv.at[spot], to).start()

    def stage_b(q):
        @pl.when(both(valid[q // 2], center))
        def _():
            fin[chunk(q)] = part[chunk(q)] + in_wait(1, q)[...]

            @pl.when(inner)
            def _():
                out_copy(q).start()

            if q % 2:
                deliver(q // 2)

    def stage_c(q):
        @pl.when(both(valid[q // 2], jnp.logical_not(center)))
        def _():
            out_copy(q).wait_recv()

            @pl.when(inner)
            def _():
                out_copy(q).start()

            if q % 2:
                deliver(q // 2)

    def inner_a(q):
        pl.when(both(valid[q // 2], inner))(functools.partial(stage_a, q))

    def edge_a(s, cond):
        @pl.when(both(edge, cond))
        def _():
            stage_a(2 * s)
            stage_a(2 * s + 1)

    @pl.when(both(first, edge))
    def _():
        for k in range(steps):
            stage_d(k)

    for s in range(slots):
        edge_a(s, both(first, near[s]))

    @pl.when(second)
    def _():
        for j in range(heads):
            pair_copy(j).wait_recv()
            high, rem = split(oth[j])
            hi[pl.ds(j * size, size), :] = high
            lo[pl.ds(j * size, size), :] = rem
        for s in range(heads):
            compute(s)

    for s in range(slots):
        edge_a(s, both(second, valid[s]))

    @pl.when(both(first, inner))
    def _():
        for k in range(steps):
            stage_d(k)

    def center_d(k):
        d_ref[d_at(c, k)] = dpart[d_in(k)] + din_wait(1, k)[...]
        spread_d(k)

    @pl.when(both(first, center))
    def _():
        for k in range(steps):
            center_d(k)

    @pl.when(first)
    def _():
        for j in range(nc):
            pair_copy(j).wait_recv()
            high, rem = split(oth[j])
            here = pl.ds(tile_rows + j * size, size)
            hi[here, :] = high
            lo[here, :] = rem
        for s in range(slots):
            pl.when(far[s])(functools.partial(compute, s))

    for s in range(slots):
        edge_a(s, both(first, far[s]))

    times = EVENTS
    events = []
    for q in range(2 * slots):
        t = times["first"] + times["step"] * q
        events.append((t, functools.partial(inner_a, q)))
        events.append((t + times["hop"], functools.partial(stage_b, q)))
        events.append((t + 2 * times["hop"], functools.partial(stage_c, q)))
    events.sort(key=lambda e: e[0])
    clock = [times["open"]]

    def advance(amount=0):
        while events and events[0][0] <= clock[0]:
            events.pop(0)[1]()
        clock[0] += amount

    @pl.when(both(first, jnp.logical_not(center)))
    def _():
        for k in range(steps):
            dout_copy(k).wait_recv()
            spread_d(k)

    @pl.when(first)
    def _():
        for k in range(steps):
            for m in range(1, nc):
                d_from(k, m).wait_recv()
                f_copy(k, m).start()

    @pl.when(second)
    def _():
        for k in range(steps):
            for m in range(nc):
                f_copy(k, m).wait_recv()

    for s in range(0, PB, BLOCK):
        e = s + BLOCK
        src = fact if s else d_ref
        inv = factor_block(work, src[s:e, s:e], lambda: advance(times["tick"]))
        invs[s // BLOCK] = inv
        if e < PB:
            u = mm(inv, src[s:e, e:], ((1,), (0,)))
            fact[s:e, e:] = u
            for j in range(e, PB, BLOCK):
                fact[j:j + BLOCK, j:] = src[j:j + BLOCK, j:] - mm(u[:, j - e:j - e + BLOCK], u[:, j - e:], ((0,), (0,)))

    @pl.when(both(first, c < heads))
    def _():
        for i in range(1, steps):
            for j in range(i):
                d_ref[i * BLOCK:(i + 1) * BLOCK, j * BLOCK:(j + 1) * BLOCK] = (
                    d_ref[j * BLOCK:(j + 1) * BLOCK, i * BLOCK:(i + 1) * BLOCK].T)

    while any(event.args[0] < 2 * heads for _, event in events):
        events.pop(0)[1]()

    @pl.when(g >= heads)
    def _():
        for j in range(heads):
            rest[:, j * size:(j + 1) * size] = fin[j]

    @pl.when(g < heads)
    def _():
        rest[...] = d_ref[rows(c * size, size), :]

    for s in range(0, PB, BLOCK):
        e = s + BLOCK
        x = mm(rest[:, s:e], invs[s // BLOCK], ((1,), (1,)))
        x_ref[:, s:e] = x
        if e < PB:
            rest[:, e:] = rest[:, e:] - mm(x, fact[s:e, e:], ((1,), (0,)))

    while events:
        events.pop(0)[1]()

    own = both(both(first, c == 0), zb < heads)

    @pl.when(own)
    def _():
        for j in range(wide):
            tin[j] = d_ref[rows(z * share, share), j * size:(j + 1) * size]

    @pl.when(jnp.logical_not(own))
    def _():
        for j in range(wide):
            remote(tin.at[j], tin.at[j], t_send.at[0, 0], t_recv.at[j], partner).wait_recv()

    folded = jnp.logical_or(c == 0, both(first, zb < heads))
    for j in range(wide):
        at = pl.ds(j * size, size)
        out_ref[:, at] = jnp.where(folded, 0.0, a_ref[rows(z * share, share), at]) + tin[j]

    holds = c == (r * nc + zb) // wide

    def n_copy(i):
        return remote(psum, nbuf.at[r * nd + z], n_send.at[i], n_recv.at[r * nd + z], device(i))

    @pl.when(holds)
    def _():
        trailing = out_ref[...]
        grow = r * tile_rows + z * share + lax.broadcasted_iota(jnp.int32, trailing.shape, 0)
        gcol = c * tile_cols + lax.broadcasted_iota(jnp.int32, trailing.shape, 1)
        squares = jnp.where(grow == gcol, trailing * trailing, 0.0)
        acc = squares.reshape(share // 8, 8, tile_cols).sum(0)
        acc = sum(acc[:, i:i + LANES] for i in range(0, tile_cols, LANES))
        psum[...] = acc
        nbuf[r * nd + z] = acc

        @pl.loop(1, devices)
        def _(i):
            n_copy(i).start()

    acc = jnp.zeros((8, LANES), F32)
    for j in range(nr * nd):
        jr, jz = j // nd, j % nd
        mine = both(holds, both(r == jr, z == jz))

        @pl.when(jnp.logical_not(mine))
        def _():
            remote(psum, nbuf.at[j], n_send.at[0], n_recv.at[j], partner).wait_recv()

        acc = acc + nbuf[j]
    n_ref[...] = jnp.sqrt(jnp.sum(acc, keepdims=True) / (tile_cols * nc))

    @pl.when(holds)
    def _():
        @pl.loop(1, devices)
        def _(i):
            n_copy(i).wait_send()

    folds(lambda copy: copy.wait_send())

    @pl.when(first)
    def _():
        for j in range(heads):
            pair_copy(j).wait_send()
        for k in range(steps):
            din_copy(k).wait_send()
            for m in range(nc):
                f_copy(k, m).wait_send()
                if m:
                    d_copy(k, m).wait_send()

            @pl.when(inner)
            def _():
                dout_copy(k).wait_send()

    @pl.when(second)
    def _():
        for j in range(nc):
            pair_copy(j).wait_send()

    for s in range(slots):
        @pl.when(valid[s])
        def _():
            for q in (2 * s, 2 * s + 1):
                in_copy(q).wait_send()

                @pl.when(inner)
                def _():
                    out_copy(q).wait_send()

        for way, (cond, src, spot, to) in enumerate(routes(s)):
            @pl.when(both(cond, jnp.logical_not(here_is(to))))
            def _():
                remote(src, tin.at[spot], t_send.at[s, way], t_recv.at[spot], to).wait_send()


def local(sizes, a_tile, panels):
    nr, nc, nd = sizes
    tile_rows, tile_cols = a_tile.shape
    k_size = panels.shape[1]
    share, size = tile_rows // nd, tile_rows // nc
    heads, wide, steps, sub = PB // size, tile_cols // size, PB // BLOCK, BLOCK // nc
    lists = plan(nr, nc, heads)
    slots = max(map(len, lists))
    vmem = pl.BlockSpec(memory_space=pltpu.VMEM)
    shape = lambda *s: jax.ShapeDtypeStruct(s, F32)
    buf = lambda *s: pltpu.VMEM(s, F32)
    dma = lambda *s: pltpu.SemaphoreType.DMA(s)
    trailing, new_panel, norm = pl.pallas_call(
        functools.partial(kernel, sizes, lists),
        out_shape=(shape(share, tile_cols), shape(size, PB), shape(1, 1)),
        in_specs=[vmem] * 2,
        out_specs=(vmem,) * 3,
        scratch_shapes=[
            pltpu.VMEM((nr * tile_rows, k_size), BF16), pltpu.VMEM((nr * tile_rows, k_size), BF16),
            buf(nc, size, k_size), buf(slots, size, size), buf(2, slots, size, size), buf(slots, size, size),
            buf(slots, size, size), buf(wide, share, size),
            buf(BLOCK, PB), buf(2, BLOCK, PB), buf(PB, PB), buf(BLOCK, PB), buf(2 * heads, size // 2, size),
            buf(8, LANES), buf(nr * nd, 8, LANES),
            buf(BLOCK, 2 * BLOCK), buf(steps, BLOCK, BLOCK), buf(PB, PB), buf(size, PB),
            dma(nc), dma(nc), dma(steps, nc), dma(steps), dma(2 * heads, nc), dma(2 * heads),
            dma(2 * slots), dma(2, 2 * slots), dma(2 * slots), dma(2 * slots),
            dma(steps), dma(2, steps), dma(steps), dma(steps), dma(steps, nc), dma(steps, nc),
            dma(steps, nc), dma(steps, nc), dma(slots, 2), dma(wide), dma(nr * nc * nd), dma(nr * nd),
        ],
        compiler_params=pltpu.CompilerParams(collective_id=0, has_side_effects=True, vmem_limit_bytes=60 << 20),
        name="trailing_update",
    )(a_tile, panels)
    return (trailing, new_panel, norm.reshape(1))


def solution(mesh):
    sizes = tuple(mesh.shape[axis] for axis in ("row", "col", "depth"))
    return jax.shard_map(
        functools.partial(local, sizes),
        mesh=mesh,
        in_specs=(P("row", "col"), P("row", "depth")),
        out_specs=(P(("row", "depth"), "col"), P(("row", "col"), None), P()),
        check_vma=False,
    )
```

```python
import functools

import jax
import jax.numpy as jnp
from jax import lax
from jax.experimental import pallas as pl
from jax.experimental.pallas import tpu as pltpu
from jax.sharding import PartitionSpec as P

PB = 512
BLOCK = 128
NB = 32
LANES = 128
TILE = 256
OPEN, TICK, HOP, NORM = 21.0, 1.05, 3.4, 37.0
ARRIVALS = ((13.0, 1.6), (23.5, 1.5), (25.5, 1.4))
EARLIEST = 17.5
SENDS = ((0.0, 0.0), (19.5, 1.4), (21.0, 1.4))
HIGHEST = lax.Precision.HIGHEST
MESH = pl.DeviceIdType.MESH
F32 = jnp.float32
BF16 = jnp.bfloat16


def split(value):
    high = value.astype(BF16)
    return high, (value - high.astype(F32)).astype(BF16)


def dot_t(left, right):
    return lax.dot_general(left, right, (((1,), (1,)), ((), ())), preferred_element_type=F32)


def product(left_hi, left_lo, right_hi, right_lo):
    return dot_t(left_hi, right_hi) + (dot_t(left_hi, right_lo) + dot_t(left_lo, right_hi))


def mm(a, b, dims):
    return lax.dot_general(a, b, (dims, ((), ())), precision=HIGHEST, preferred_element_type=F32)


def factor_block(work, block, advance):
    work[:, :BLOCK] = block
    diag = lax.broadcasted_iota(jnp.int32, (BLOCK, BLOCK), 0) == lax.broadcasted_iota(jnp.int32, (BLOCK, BLOCK), 1)
    work[:, BLOCK:] = jnp.where(diag, 1.0, 0.0)
    sub = lax.broadcasted_iota(jnp.int32, (NB, BLOCK), 0)
    for j in range(0, BLOCK, NB):
        left = work[j:j + NB, :BLOCK]
        right = work[j:j + NB, BLOCK:]
        advance()
        lanes = [jnp.broadcast_to(left[:, j + k:j + k + 1], (NB, BLOCK)) for k in range(NB)]
        for k in range(NB):
            inv = lax.rsqrt(lanes[k][k:k + 1])
            col = lanes[k] * inv
            for i in range(k + 1, NB):
                lanes[i] = lanes[i] - col * col[i:i + 1]
            row_l = left[k:k + 1] * inv
            row_r = right[k:k + 1] * inv
            below = jnp.where(sub > k, col, 0.0)
            left = jnp.where(sub == k, row_l, left - below * row_l)
            right = jnp.where(sub == k, row_r, right - below * row_r)
        work[j:j + NB, :BLOCK] = left
        work[j:j + NB, BLOCK:] = right
        if j + NB < BLOCK:
            both = jnp.concatenate([left, right], axis=1)
            work[j + NB:, :] = work[j + NB:, :] - mm(left[:, j + NB:], both, ((0,), (0,)))
    return work[:, BLOCK:]


def plan(nr, nc, heads):
    lists = [[] for _ in range(nr * nc)]
    for g in range(heads, nr * nc):
        lists[g] = [(g, g)] + [(g, j) for j in range(heads)]
    for low in range(heads, nr * nc):
        for high in range(low + 1, nr * nc):
            able = [g for g in range(nr * nc) if g < nc or g // nc == low // nc]
            best = min(able, key=lambda g: (len(lists[g]), g not in (low, high), g))
            lists[best].append((low, high) if best == low else (high, low))
    return lists


def kernel(sizes, lists, a_hbm, p_hbm, out_ref, x_ref, n_ref, *scratch):
    nr, nc, nd = sizes
    (a_ref, p_ref, hi, lo, oth, part, rin, fin, turned, tin, dpart, drin, d_ref, adbuf, acbuf, psum, nbuf,
     work, invs, fact, rest,
     load, pair_send, pair_recv, ad_send, ad_recv, ac_send, ac_recv, in_send, in_recv, out_send, out_recv,
     di_send, di_recv, do_send, do_recv, d_send, d_recv, f_send, f_recv, t_send, t_recv, n_send, n_recv) = scratch
    tile_rows, tile_cols = a_ref.shape
    size = tile_rows // nc
    half = size // 2
    heads = PB // size
    wide = tile_cols // size
    share = tile_rows // nd
    sub = BLOCK // nc
    steps = PB // BLOCK
    slots = max(map(len, lists))
    devices = nr * nc * nd
    r, c, z = lax.axis_index("row"), lax.axis_index("col"), lax.axis_index("depth")
    g = r * nc + c
    mid = nd // 2
    low = z < mid
    center = jnp.logical_or(z == mid - 1, z == mid)
    edge = jnp.logical_or(z == 0, z == nd - 1)
    inner = jnp.logical_not(edge)
    side = jnp.where(center, 1, 0)
    inward = jnp.where(low, z + 1, z - 1)
    outward = jnp.where(low, z - 1, z + 1)
    zb = z * share // size
    zo = lax.rem(z * share, size)
    first, second = r == 0, r != 0
    partner = (1 - r, c, z)
    both = jnp.logical_and

    def pick(values):
        result = jnp.int32(values[0])
        for i, value in enumerate(values[1:], 1):
            result = jnp.where(g == i, value, result)
        return result

    xs = [pick([l[s][0] if s < len(l) else 0 for l in lists]) for s in range(slots)]
    ys = [pick([l[s][1] if s < len(l) else 0 for l in lists]) for s in range(slots)]
    counts = pick([len(l) for l in lists])
    valid = [s < counts for s in range(slots)]
    near = [both(valid[s], both(xs[s] // nc == r, ys[s] // nc == r)) for s in range(slots)]
    far = [both(valid[s], jnp.logical_not(both(xs[s] // nc == r, ys[s] // nc == r))) for s in range(slots)]

    def remote(src, dst, send, recv, device):
        return pltpu.make_async_remote_copy(
            src_ref=src, dst_ref=dst, send_sem=send, recv_sem=recv, device_id=device, device_id_type=MESH)

    def rows(start, count):
        return pl.ds(pl.multiple_of(start, count), count)

    def p_load(t):
        at = pl.ds(t * TILE, TILE)
        return pltpu.make_async_copy(p_hbm.at[at, :], p_ref.at[at, :], load.at[t])

    a_load = pltpu.make_async_copy(a_hbm, a_ref, load.at[tile_rows // TILE])
    for t in range(tile_rows // TILE):
        p_load(t).start()
    a_load.start()

    barrier = pltpu.get_barrier_semaphore()
    me = g * nd + z

    def device(i):
        there = lax.rem(me + i, devices)
        return (there // (nc * nd), lax.rem(there // nd, nc), lax.rem(there, nd))

    @pl.loop(0, nd)
    def _(k):
        depth = lax.rem(z + k, nd)
        for i in range(nr * nc):
            to = (r if i < nc else 1 - r, lax.rem(c + i % nc, nc), depth)
            if i:
                pl.semaphore_signal(barrier, inc=1, device_id=to, device_id_type=MESH)
            else:
                @pl.when(k > 0)
                def _():
                    pl.semaphore_signal(barrier, inc=1, device_id=to, device_id_type=MESH)

    def split_own(t):
        p_load(t).wait()
        high, rem = split(p_ref[pl.ds(t * TILE, TILE), :])
        here = rows(r * tile_rows + t * TILE, TILE)
        hi[here, :] = high
        lo[here, :] = rem

    for t in range(PB // TILE):
        split_own(t)

    def compute(s):
        a, b = rows(xs[s] * size, size), rows(ys[s] * size, size)
        part[s] = -product(hi[a, :], lo[a, :], hi[b, :], lo[b, :])

    @pl.when(first)
    def _():
        at = [pl.ds(pl.multiple_of(k * BLOCK + c * sub, sub), sub) for k in range(steps)]
        left_hi = jnp.concatenate([hi[i, :] for i in at], axis=0)
        left_lo = jnp.concatenate([lo[i, :] for i in at], axis=0)
        dpart[...] = -product(left_hi, left_lo, hi[:PB, :], lo[:PB, :])

    for t in range(PB // TILE, tile_rows // TILE):
        split_own(t)
    a_load.wait()
    for s in range(slots):
        pl.when(near[s])(functools.partial(compute, s))

    pl.semaphore_wait(barrier, devices - 1)

    def pair_copy(j):
        return remote(p_ref.at[rows(j * size, size), :], oth.at[j], pair_send.at[j], pair_recv.at[j], partner)

    def d_fold(k):
        return mid - 1 + k % 2

    def c_fold(q):
        return (mid - 1, mid, 0, nd - 1)[q % 4]

    def d_at(col, k):
        return (pl.ds(pl.multiple_of(k * BLOCK + col * sub, sub), sub), pl.ds(k * BLOCK, PB - k * BLOCK))

    def d_in(k):
        return (pl.ds(k * sub, sub), pl.ds(k * BLOCK, PB - k * BLOCK))

    def ad_copy(k, to):
        return remote(a_ref.at[d_at(to, k)], adbuf.at[d_in(k)], ad_send.at[k, to], ad_recv.at[k], (r, to, z))

    def ac_at(col, q):
        return (rows(col * size + q % 2 * half, half), pl.ds((q // 2 - 1) * size, size))

    def ac_copy(q, to):
        return remote(a_ref.at[ac_at(to, q)], acbuf.at[q - 2], ac_send.at[q - 2, to], ac_recv.at[q - 2], (r, to, z))

    def d_folds(act):
        for k in range(steps):
            @pl.when(both(both(first, c == 0), z == d_fold(k)))
            def _():
                for to in range(1, nc):
                    act(ad_copy(k, to))

    def c_folds(act):
        for q in range(2, 2 + 2 * heads):
            for to in range(1, nc):
                @pl.when(both(both(c == 0, z == c_fold(q)), r * nc + to >= heads))
                def _():
                    act(ac_copy(q, to))

    d_folds(lambda copy: copy.start())

    def din_copy(k):
        return remote(dpart.at[d_in(k)], drin.at[(side,) + d_in(k)], di_send.at[k], di_recv.at[side, k], (r, c, inward))

    def din_wait(at, k):
        here = drin.at[(at,) + d_in(k)]
        remote(here, here, di_send.at[k], di_recv.at[at, k], (r, c, inward)).wait_recv()
        return here

    def stage_d(k):
        @pl.when(inner)
        def _():
            dpart[d_in(k)] = dpart[d_in(k)] + din_wait(0, k)[...]

        @pl.when(z == d_fold(k))
        def _():
            @pl.when(c == 0)
            def _():
                dpart[d_in(k)] = dpart[d_in(k)] + a_ref[d_at(0, k)]

            @pl.when(c != 0)
            def _():
                ad_copy(k, 1).wait_recv()
                dpart[d_in(k)] = dpart[d_in(k)] + adbuf[d_in(k)]

        din_copy(k).start()

    def dout_copy(k):
        here = d_ref.at[d_at(c, k)]
        return remote(here, here, do_send.at[k], do_recv.at[k], (r, c, outward))

    def d_copy(k, m):
        here = d_ref.at[d_at(c, k)]
        return remote(here, here, d_send.at[k, m], d_recv.at[k, m], (r, lax.rem(c + m, nc), z))

    def d_from(k, m):
        there = d_ref.at[d_at(lax.rem(c - m + nc, nc), k)]
        return remote(there, there, d_send.at[k, m], d_recv.at[k, m], (r, lax.rem(c + m, nc), z))

    def f_copy(k, m):
        there = d_ref.at[d_at(lax.rem(c - m + nc, nc), k)]
        return remote(there, there, f_send.at[k, m], f_recv.at[k, m], partner)

    def spread_d(k):
        @pl.when(inner)
        def _():
            dout_copy(k).start()

        for m in range(1, nc):
            d_copy(k, m).start()
        f_copy(k, 0).start()

    def chunk(q):
        return (q // 2, pl.ds(q % 2 * half, half), slice(None))

    def in_copy(q):
        return remote(part.at[chunk(q)], rin.at[(side,) + chunk(q)], in_send.at[q], in_recv.at[side, q], (r, c, inward))

    def in_wait(at, q):
        here = rin.at[(at,) + chunk(q)]
        remote(here, here, in_send.at[q], in_recv.at[at, q], (r, c, inward)).wait_recv()
        return here

    def out_copy(q):
        here = fin.at[chunk(q)]
        return remote(here, here, out_send.at[q], out_recv.at[q], (r, c, outward))

    def stage_a(q):
        @pl.when(inner)
        def _():
            part[chunk(q)] = part[chunk(q)] + in_wait(0, q)[...]

        if 0 < q // 2 <= heads:
            @pl.when(both(g >= heads, z == c_fold(q)))
            def _():
                @pl.when(c == 0)
                def _():
                    part[chunk(q)] = part[chunk(q)] + a_ref[ac_at(0, q)]

                @pl.when(c != 0)
                def _():
                    ac_copy(q, 1).wait_recv()
                    part[chunk(q)] = part[chunk(q)] + acbuf[q - 2]

        in_copy(q).start()

    def here_is(device):
        return both(device[0] == r, device[1] == c)

    def routes(s):
        x, y = xs[s], ys[s]
        straight = (x // nc, y // wide, z)
        across = (y // nc, x // wide, z)
        return (
            (both(valid[s], zb == lax.rem(x, nc)), fin.at[s, rows(zo, share), :], lax.rem(y, wide), straight),
            (both(both(valid[s], x != y), zb == lax.rem(y, nc)), turned.at[s, rows(zo, share), :], lax.rem(x, wide), across),
        )

    def deliver(s):
        for way, (cond, src, spot, to) in enumerate(routes(s)):
            @pl.when(cond)
            def _():
                if way:
                    turned[s] = fin[s].T

                @pl.when(here_is(to))
                def _():
                    pltpu.make_async_copy(src, tin.at[spot], t_recv.at[spot]).start()

                @pl.when(jnp.logical_not(here_is(to)))
                def _():
                    remote(src, tin.at[spot], t_send.at[s, way], t_recv.at[spot], to).start()

    def stage_b(q, member):
        @pl.when(both(both(valid[q // 2], member), center))
        def _():
            fin[chunk(q)] = part[chunk(q)] + in_wait(1, q)[...]

            @pl.when(inner)
            def _():
                out_copy(q).start()

            if q % 2:
                deliver(q // 2)

    def stage_c(q, member):
        @pl.when(both(both(valid[q // 2], member), jnp.logical_not(center)))
        def _():
            out_copy(q).wait_recv()

            @pl.when(inner)
            def _():
                out_copy(q).start()

            if q % 2:
                deliver(q // 2)

    def edge_send(q, member):
        pl.when(both(both(valid[q // 2], member), edge))(functools.partial(stage_a, q))

    def inner_a(q, member):
        pl.when(both(both(valid[q // 2], member), inner))(functools.partial(stage_a, q))

    def edge_a(s, cond):
        @pl.when(both(edge, cond))
        def _():
            stage_a(2 * s)
            stage_a(2 * s + 1)

    @pl.when(both(first, edge))
    def _():
        for k in range(steps):
            stage_d(k)

    @pl.when(first)
    def _():
        for j in range(heads):
            pair_copy(j).start()

    @pl.when(second)
    def _():
        for j in range(nc):
            pair_copy(j).start()

    c_folds(lambda copy: copy.start())
    edge_a(0, both(second, near[0]))

    @pl.when(second)
    def _():
        for j in range(heads):
            pair_copy(j).wait_recv()
            high, rem = split(oth[j])
            hi[pl.ds(j * size, size), :] = high
            lo[pl.ds(j * size, size), :] = rem
        for s in range(1, 1 + heads):
            compute(s)

    for s in range(1, slots):
        edge_a(s, both(second, valid[s]))

    def center_d(k):
        @pl.when(center)
        def _():
            d_ref[d_at(c, k)] = dpart[d_in(k)] + din_wait(1, k)[...]
            spread_d(k)

    @pl.when(both(first, inner))
    def _():
        for k in range(steps):
            stage_d(k)
            if k:
                center_d(k - 1)
        center_d(steps - 1)

    def outer_d(k):
        @pl.when(both(first, jnp.logical_not(center)))
        def _():
            dout_copy(k).wait_recv()
            spread_d(k)

    def gather_d(k):
        @pl.when(first)
        def _():
            for m in range(1, nc):
                d_from(k, m).wait_recv()
                f_copy(k, m).start()

    def arrive_d(k):
        @pl.when(second)
        def _():
            for m in range(nc):
                f_copy(k, m).wait_recv()

    own = both(both(first, c == 0), zb < heads)
    holds = c == (r * nc + zb) // wide
    spot = lax.rem(r * nc + zb, wide)

    def t_wait(j):
        remote(tin.at[j], tin.at[j], t_send.at[0, 0], t_recv.at[j], partner).wait_recv()

    def n_copy(i):
        return remote(psum, nbuf.at[r * nd + z], n_send.at[i], n_recv.at[r * nd + z], device(i))

    def norm_part():
        for j in range(wide):
            pl.when(both(both(holds, jnp.logical_not(own)), spot == j))(functools.partial(t_wait, j))

        @pl.when(holds)
        def _():
            base = a_ref[rows(z * share, share), rows(spot * size, size)]
            block = jnp.where(own, d_ref[rows(lax.rem(z * share, PB), share), rows(lax.rem(r * nc + zb, heads) * size, size)], base + tin[spot])
            row = zo + lax.broadcasted_iota(jnp.int32, block.shape, 0)
            squares = jnp.where(row == lax.broadcasted_iota(jnp.int32, block.shape, 1), block * block, 0.0)
            acc = squares.reshape(share // 8, 8, size).sum(0)
            acc = sum(acc[:, i:i + LANES] for i in range(0, size, LANES))
            psum[...] = acc
            nbuf[r * nd + z] = acc

            @pl.loop(1, devices)
            def _(i):
                n_copy(i).start()

    members = (second, both(first, g >= heads), g < heads)
    events = []
    for member, (arrive, step), (send, gap) in zip(members, ARRIVALS, SENDS):
        for q in range(2 * slots):
            for when, stage in enumerate((inner_a, stage_b, stage_c)):
                events.append((arrive + step * q + when * HOP, q // 2 <= heads, functools.partial(stage, q, member)))
            if send:
                events.append((send + gap * q, q // 2 <= heads, functools.partial(edge_send, q, member)))
    for k in range(1, steps):
        events.append((OPEN + k, True, functools.partial(gather_d, k)))
    events.append((NORM, False, norm_part))
    events.sort(key=lambda e: e[0])

    def advance(now):
        while events and events[0][0] <= now:
            events.pop(0)[2]()

    advance(EARLIEST)
    for k in range(steps):
        outer_d(k)

    @pl.when(first)
    def _():
        for j in range(nc):
            pair_copy(j).wait_recv()
            high, rem = split(oth[j])
            here = pl.ds(tile_rows + j * size, size)
            hi[here, :] = high
            lo[here, :] = rem
        for s in range(slots):
            pl.when(far[s])(functools.partial(compute, s))

    gather_d(0)
    arrive_d(0)
    clock = [OPEN]

    def tick():
        advance(clock[0])
        clock[0] += TICK

    for s in range(0, PB, BLOCK):
        e = s + BLOCK
        src = fact if s else d_ref
        inv = factor_block(work, src[s:e, s:e], tick)
        invs[s // BLOCK] = inv
        if s == 0:
            for k in range(1, steps):
                arrive_d(k)
        if e < PB:
            u = mm(inv, src[s:e, e:], ((1,), (0,)))
            fact[s:e, e:] = u
            for j in range(e, PB, BLOCK):
                fact[j:j + BLOCK, j:] = src[j:j + BLOCK, j:] - mm(u[:, j - e:j - e + BLOCK], u[:, j - e:], ((0,), (0,)))

    @pl.when(both(first, c < heads))
    def _():
        for i in range(1, steps):
            for j in range(i):
                d_ref[i * BLOCK:(i + 1) * BLOCK, j * BLOCK:(j + 1) * BLOCK] = (
                    d_ref[j * BLOCK:(j + 1) * BLOCK, i * BLOCK:(i + 1) * BLOCK].T)

    @pl.when(own)
    def _():
        for j in range(wide):
            tin[j] = d_ref[rows(z * share, share), j * size:(j + 1) * size]

    while any(event[1] for event in events):
        events.pop(0)[2]()

    @pl.when(g >= heads)
    def _():
        for j in range(heads):
            rest[:, j * size:(j + 1) * size] = fin[1 + j]

    @pl.when(g < heads)
    def _():
        rest[...] = d_ref[rows(c * size, size), :]

    for s in range(0, PB, BLOCK):
        e = s + BLOCK
        x = mm(rest[:, s:e], invs[s // BLOCK], ((1,), (1,)))
        x_ref[:, s:e] = x
        if e < PB:
            rest[:, e:] = rest[:, e:] - mm(x, fact[s:e, e:], ((1,), (0,)))

    while events:
        events.pop(0)[2]()

    @pl.when(jnp.logical_not(own))
    def _():
        for j in range(wide):
            pl.when(jnp.logical_not(both(holds, spot == j)))(functools.partial(t_wait, j))

    folded = jnp.logical_or(c == 0, both(first, zb < heads))
    for j in range(wide):
        at = pl.ds(j * size, size)
        out_ref[:, at] = jnp.where(folded, 0.0, a_ref[rows(z * share, share), at]) + tin[j]

    acc = jnp.zeros((8, LANES), F32)
    for j in range(nr * nd):
        jr, jz = j // nd, j % nd
        mine = both(holds, both(r == jr, z == jz))

        @pl.when(jnp.logical_not(mine))
        def _():
            remote(psum, nbuf.at[j], n_send.at[0], n_recv.at[j], partner).wait_recv()

        acc = acc + nbuf[j]
    n_ref[...] = jnp.sqrt(jnp.sum(acc, keepdims=True) / (tile_cols * nc))

    @pl.when(holds)
    def _():
        @pl.loop(1, devices)
        def _(i):
            n_copy(i).wait_send()

    d_folds(lambda copy: copy.wait_send())
    c_folds(lambda copy: copy.wait_send())

    @pl.when(first)
    def _():
        for j in range(heads):
            pair_copy(j).wait_send()
        for k in range(steps):
            din_copy(k).wait_send()
            for m in range(nc):
                f_copy(k, m).wait_send()
                if m:
                    d_copy(k, m).wait_send()

            @pl.when(inner)
            def _():
                dout_copy(k).wait_send()

    @pl.when(second)
    def _():
        for j in range(nc):
            pair_copy(j).wait_send()

    for s in range(slots):
        @pl.when(valid[s])
        def _():
            for q in (2 * s, 2 * s + 1):
                in_copy(q).wait_send()

                @pl.when(inner)
                def _():
                    out_copy(q).wait_send()

        for way, (cond, src, spot, to) in enumerate(routes(s)):
            @pl.when(both(cond, jnp.logical_not(here_is(to))))
            def _():
                remote(src, tin.at[spot], t_send.at[s, way], t_recv.at[spot], to).wait_send()


def local(sizes, a_tile, panels):
    nr, nc, nd = sizes
    tile_rows, tile_cols = a_tile.shape
    k_size = panels.shape[1]
    share, size = tile_rows // nd, tile_rows // nc
    heads, wide, steps, sub = PB // size, tile_cols // size, PB // BLOCK, BLOCK // nc
    lists = plan(nr, nc, heads)
    slots = max(map(len, lists))
    vmem = pl.BlockSpec(memory_space=pltpu.VMEM)
    buf = lambda *s: pltpu.VMEM(s, F32)
    dma = lambda *s: pltpu.SemaphoreType.DMA(s)
    trailing, new_panel, norm = pl.pallas_call(
        functools.partial(kernel, sizes, lists),
        out_shape=(buf(share, tile_cols), buf(size, PB), buf(1, 1)),
        in_specs=[pl.BlockSpec(memory_space=pl.ANY)] * 2,
        out_specs=(vmem,) * 3,
        scratch_shapes=[
            buf(tile_rows, tile_cols), buf(tile_rows, k_size),
            pltpu.VMEM((nr * tile_rows, k_size), BF16), pltpu.VMEM((nr * tile_rows, k_size), BF16),
            buf(nc, size, k_size), buf(slots, size, size), buf(2, slots, size, size), buf(slots, size, size),
            buf(slots, size, size), buf(wide, share, size),
            buf(BLOCK, PB), buf(2, BLOCK, PB), buf(PB, PB), buf(BLOCK, PB), buf(2 * heads, size // 2, size),
            buf(8, LANES), buf(nr * nd, 8, LANES),
            buf(BLOCK, 2 * BLOCK), buf(steps, BLOCK, BLOCK), buf(PB, PB), buf(size, PB),
            dma(tile_rows // TILE + 1), dma(nc), dma(nc), dma(steps, nc), dma(steps), dma(2 * heads, nc), dma(2 * heads),
            dma(2 * slots), dma(2, 2 * slots), dma(2 * slots), dma(2 * slots),
            dma(steps), dma(2, steps), dma(steps), dma(steps), dma(steps, nc), dma(steps, nc),
            dma(steps, nc), dma(steps, nc), dma(slots, 2), dma(wide), dma(nr * nc * nd), dma(nr * nd),
        ],
        compiler_params=pltpu.CompilerParams(collective_id=0, has_side_effects=True, vmem_limit_bytes=62 << 20),
        name="trailing_update",
    )(a_tile, panels)
    return (trailing, new_panel, norm.reshape(1))


def solution(mesh):
    sizes = tuple(mesh.shape[axis] for axis in ("row", "col", "depth"))
    return jax.shard_map(
        functools.partial(local, sizes),
        mesh=mesh,
        in_specs=(P("row", "col"), P("row", "depth")),
        out_specs=(P(("row", "depth"), "col"), P(("row", "col"), None), P()),
        check_vma=False,
    )
```

```python
import functools

import jax
import jax.numpy as jnp
from jax import lax
from jax.experimental import pallas as pl
from jax.experimental.pallas import tpu as pltpu
from jax.sharding import PartitionSpec as P

PB = 512
BLOCK = 128
NB = 32
LANES = 128
TILE = 256
OPEN, TICK, HOP, NORM = 19.5, 1.0, 3.4, 34.0
ARRIVALS = ((12.5, 1.6), (23.0, 1.4), (23.0, 1.4))
EARLIEST = 16.0
SENDS = ((0.0, 0.0), (18.1, 1.4), (18.1, 1.4))
MESH = pl.DeviceIdType.MESH
F32 = jnp.float32
BF16 = jnp.bfloat16


def split(value):
    high = value.astype(BF16)
    return high, (value - high.astype(F32)).astype(BF16)


def dot_t(left, right):
    return lax.dot_general(left, right, (((1,), (1,)), ((), ())), preferred_element_type=F32)


def product(left_hi, left_lo, right_hi, right_lo):
    return dot_t(left_hi, right_hi) + (dot_t(left_hi, right_lo) + dot_t(left_lo, right_hi))


def mm(a, b, dims):
    a_hi, a_lo = split(a)
    b_hi, b_lo = split(b)
    dot = lambda x, y: lax.dot_general(x, y, (dims, ((), ())), preferred_element_type=F32)
    return dot(a_hi, b_hi) + (dot(a_hi, b_lo) + dot(a_lo, b_hi))


def factor_block(work, block, advance):
    work[:, :BLOCK] = block
    diag = lax.broadcasted_iota(jnp.int32, (BLOCK, BLOCK), 0) == lax.broadcasted_iota(jnp.int32, (BLOCK, BLOCK), 1)
    work[:, BLOCK:] = jnp.where(diag, 1.0, 0.0)
    sub = lax.broadcasted_iota(jnp.int32, (NB, BLOCK), 0)
    for j in range(0, BLOCK, NB):
        left = work[j:j + NB, :BLOCK]
        right = work[j:j + NB, BLOCK:]
        advance()
        lanes = [jnp.broadcast_to(left[:, j + k:j + k + 1], (NB, BLOCK)) for k in range(NB)]
        for k in range(NB):
            inv = lax.rsqrt(lanes[k][k:k + 1])
            col = lanes[k] * inv
            for i in range(k + 1, NB):
                lanes[i] = lanes[i] - col * col[i:i + 1]
            row_l = left[k:k + 1] * inv
            row_r = right[k:k + 1] * inv
            below = jnp.where(sub > k, col, 0.0)
            left = jnp.where(sub == k, row_l, left - below * row_l)
            right = jnp.where(sub == k, row_r, right - below * row_r)
        work[j:j + NB, :BLOCK] = left
        work[j:j + NB, BLOCK:] = right
        if j + NB < BLOCK:
            both = jnp.concatenate([left, right], axis=1)
            work[j + NB:, :] = work[j + NB:, :] - mm(left[:, j + NB:], both, ((0,), (0,)))
    return work[:, BLOCK:]


def plan(nr, nc, heads):
    lists = [[] for _ in range(nr * nc)]
    for g in range(heads, nr * nc):
        lists[g] = [(g, g)] + [(g, j) for j in range(heads)]
    for low in range(heads, nr * nc):
        for high in range(low + 1, nr * nc):
            able = [g for g in range(nr * nc) if g < nc or g // nc == low // nc]
            best = min(able, key=lambda g: (len(lists[g]), g not in (low, high), g))
            lists[best].append((low, high) if best == low else (high, low))
    return lists


def kernel(sizes, lists, a_hbm, p_hbm, out_ref, x_ref, n_ref, *scratch):
    nr, nc, nd = sizes
    (a_ref, p_ref, hi, lo, oth, part, rin, fin, turned, tin, drin, d_ref, adbuf, acbuf, psum, nbuf, spent,
     work, invs, fact, rest,
     load, pair_send, pair_recv, ad_send, ad_recv, ac_send, ac_recv, in_send, in_recv, out_send, out_recv,
     di_send, di_recv, do_send, do_recv, d_send, d_recv, f_send, f_recv, t_send, t_recv, n_send, n_recv) = scratch
    tile_rows, tile_cols = a_ref.shape
    size = tile_rows // nc
    half = size // 2
    heads = PB // size
    wide = tile_cols // size
    share = tile_rows // nd
    sub = BLOCK // nc
    steps = PB // BLOCK
    slots, base = max(map(len, lists)), min(map(len, lists))
    unit = sub * (steps + 1) // 2
    devices = nr * nc * nd
    r, c, z = lax.axis_index("row"), lax.axis_index("col"), lax.axis_index("depth")
    g = r * nc + c
    mid = nd // 2
    low = z < mid
    center = jnp.logical_or(z == mid - 1, z == mid)
    edge = jnp.logical_or(z == 0, z == nd - 1)
    inner = jnp.logical_not(edge)
    side = jnp.where(center, 1, 0)
    inward = jnp.where(low, z + 1, z - 1)
    outward = jnp.where(low, z - 1, z + 1)
    zb = z * share // size
    zo = lax.rem(z * share, size)
    first, second = r == 0, r != 0
    partner = (1 - r, c, z)
    both = jnp.logical_and

    def pick(values):
        result = jnp.int32(values[0])
        for i, value in enumerate(values[1:], 1):
            result = jnp.where(g == i, value, result)
        return result

    xs = [pick([l[s][0] if s < len(l) else 0 for l in lists]) for s in range(slots)]
    ys = [pick([l[s][1] if s < len(l) else 0 for l in lists]) for s in range(slots)]
    counts = pick([len(l) for l in lists])
    valid = [s < counts for s in range(slots)]
    near = [both(valid[s], both(xs[s] // nc == r, ys[s] // nc == r)) for s in range(slots)]
    far = [both(valid[s], jnp.logical_not(both(xs[s] // nc == r, ys[s] // nc == r))) for s in range(slots)]

    def remote(src, dst, send, recv, device):
        return pltpu.make_async_remote_copy(
            src_ref=src, dst_ref=dst, send_sem=send, recv_sem=recv, device_id=device, device_id_type=MESH)

    def rows(start, count):
        return pl.ds(pl.multiple_of(start, count), count)

    def p_load(t):
        at = pl.ds(t * TILE, TILE)
        return pltpu.make_async_copy(p_hbm.at[at, :], p_ref.at[at, :], load.at[t])

    a_load = pltpu.make_async_copy(a_hbm, a_ref, load.at[tile_rows // TILE])
    for t in range(tile_rows // TILE):
        p_load(t).start()
    a_load.start()

    barrier = pltpu.get_barrier_semaphore()
    me = g * nd + z

    def device(i):
        there = lax.rem(me + i, devices)
        return (there // (nc * nd), lax.rem(there // nd, nc), lax.rem(there, nd))

    @pl.loop(0, nd)
    def _(k):
        depth = lax.rem(z + k, nd)
        for i in range(nr * nc):
            to = (r if i < nc else 1 - r, lax.rem(c + i % nc, nc), depth)
            if i:
                pl.semaphore_signal(barrier, inc=1, device_id=to, device_id_type=MESH)
            else:
                @pl.when(k > 0)
                def _():
                    pl.semaphore_signal(barrier, inc=1, device_id=to, device_id_type=MESH)

    def split_own(t):
        p_load(t).wait()
        high, rem = split(p_ref[pl.ds(t * TILE, TILE), :])
        here = rows(r * tile_rows + t * TILE, TILE)
        hi[here, :] = high
        lo[here, :] = rem

    for t in range(PB // TILE):
        split_own(t)

    def compute(s):
        a, b = rows(xs[s] * size, size), rows(ys[s] * size, size)
        part[s] = -product(hi[a, :], lo[a, :], hi[b, :], lo[b, :])

    @pl.when(first)
    def _():
        at = [pl.ds(pl.multiple_of(k * BLOCK + c * sub, sub), sub) for k in range(steps)]
        left_hi = jnp.concatenate([hi[i, :] for i in at], axis=0)
        left_lo = jnp.concatenate([lo[i, :] for i in at], axis=0)
        drin[z] = -product(left_hi, left_lo, hi[:PB, :], lo[:PB, :])

    for t in range(PB // TILE, tile_rows // TILE):
        split_own(t)
    a_load.wait()
    for s in range(slots):
        pl.when(near[s])(functools.partial(compute, s))

    pl.semaphore_wait(barrier, devices - 1)

    def pair_copy(j):
        return remote(p_ref.at[rows(j * size, size), :], oth.at[j], pair_send, pair_recv, partner)

    def pair_all(count):
        return remote(oth.at[pl.ds(0, count)], oth.at[pl.ds(0, count)], pair_send, pair_recv, partner)

    def rows_of(count):
        return fact.at[pl.ds(0, count), :]

    def c_fold(q):
        return (mid - 1, mid, 0, nd - 1)[q % 4]

    def d_at(col, k):
        return (pl.ds(pl.multiple_of(k * BLOCK + col * sub, sub), sub), pl.ds(k * BLOCK, PB - k * BLOCK))

    def d_in(k):
        return (pl.ds(k * sub, sub), pl.ds(k * BLOCK, PB - k * BLOCK))

    def ad_copy(k, to):
        return remote(a_ref.at[d_at(to, k)], adbuf.at[d_in(k)], ad_send, ad_recv.at[k], (r, to, z))

    def ac_at(col, q):
        return (rows(col * size + q % 2 * half, half), pl.ds((q // 2 - 1) * size, size))

    def ac_copy(q, to):
        return remote(a_ref.at[ac_at(to, q)], acbuf.at[q - 2], ac_send.at[(q - 2) // 2, to], ac_recv.at[q - 2], (r, to, z))

    @pl.when(both(both(first, c == 0), center))
    def _():
        for k in range(steps):
            for to in range(1, nc):
                ad_copy(k, to).start()

    def c_folds(act):
        for q in range(2, 2 + 2 * heads):
            for to in range(1, nc):
                @pl.when(both(both(c == 0, z == c_fold(q)), r * nc + to >= heads))
                def _():
                    act(ac_copy(q, to))

    def din_copy(k, to):
        here = drin.at[(z,) + d_in(k)]
        return remote(here, here, di_send, di_recv.at[k], (r, c, to))

    def stage_d(k):
        for to in (mid - 1, mid):
            pl.when(z != to)(din_copy(k, to).start)

    def dout_copy(k, to):
        here = d_ref.at[d_at(c, k)]
        return remote(here, here, do_send, do_recv.at[k], (r, c, to))

    def d_copy(k, m):
        here = d_ref.at[d_at(c, k)]
        return remote(here, here, d_send, d_recv.at[k], (r, lax.rem(c + m, nc), z))

    def d_rows(k, count):
        return d_ref.at[pl.ds(k * BLOCK, count), pl.ds(k * BLOCK, PB - k * BLOCK)]

    def f_copy(k, m):
        there = d_ref.at[d_at(lax.rem(c - m + nc, nc), k)]
        return remote(there, there, f_send, f_recv.at[k], partner)

    def spread_d(k):
        for m in range(1, nc):
            d_copy(k, m).start()
        f_copy(k, 0).start()

    def chunk(q):
        return (q // 2, pl.ds(q % 2 * half, half), slice(None))

    def in_copy(q):
        return remote(part.at[chunk(q)], rin.at[(side,) + chunk(q)], in_send.at[max(0, q // 2 - base + 1)], in_recv.at[side, q], (r, c, inward))

    def in_wait(at, q):
        here = rin.at[(at,) + chunk(q)]
        remote(here, here, in_send.at[0], in_recv.at[at, q], (r, c, inward)).wait_recv()
        return here

    def out_copy(q):
        here = fin.at[chunk(q)]
        return remote(here, here, out_send.at[max(0, q // 2 - base + 1)], out_recv.at[q], (r, c, outward))

    def stage_a(q):
        @pl.when(inner)
        def _():
            part[chunk(q)] = part[chunk(q)] + in_wait(0, q)[...]

        if 0 < q // 2 <= heads:
            @pl.when(both(g >= heads, z == c_fold(q)))
            def _():
                @pl.when(c == 0)
                def _():
                    part[chunk(q)] = part[chunk(q)] + a_ref[ac_at(0, q)]

                @pl.when(c != 0)
                def _():
                    ac_copy(q, 1).wait_recv()
                    part[chunk(q)] = part[chunk(q)] + acbuf[q - 2]

        in_copy(q).start()

    def here_is(device):
        return both(device[0] == r, device[1] == c)

    def routes(s):
        x, y = xs[s], ys[s]
        straight = (x // nc, y // wide, z)
        across = (y // nc, x // wide, z)
        return (
            (both(valid[s], zb == lax.rem(x, nc)), fin.at[s, rows(zo, share), :], lax.rem(y, wide), straight),
            (both(both(valid[s], x != y), zb == lax.rem(y, nc)), turned.at[s, rows(zo, share), :], lax.rem(x, wide), across),
        )

    def deliver(s):
        for way, (cond, src, spot, to) in enumerate(routes(s)):
            @pl.when(cond)
            def _():
                if way:
                    turned[s] = fin[s].T

                @pl.when(here_is(to))
                def _():
                    pltpu.make_async_copy(src, tin.at[spot], t_recv.at[spot]).start()

                @pl.when(jnp.logical_not(here_is(to)))
                def _():
                    remote(src, tin.at[spot], t_send.at[s, way], t_recv.at[spot], to).start()

    def stage_b(q, member):
        @pl.when(both(both(valid[q // 2], member), center))
        def _():
            fin[chunk(q)] = part[chunk(q)] + in_wait(1, q)[...]

            @pl.when(inner)
            def _():
                out_copy(q).start()

            if q % 2:
                deliver(q // 2)

    def stage_c(q, member):
        @pl.when(both(both(valid[q // 2], member), jnp.logical_not(center)))
        def _():
            out_copy(q).wait_recv()

            @pl.when(inner)
            def _():
                out_copy(q).start()

            if q % 2:
                deliver(q // 2)

    def edge_send(q, member):
        pl.when(both(both(valid[q // 2], member), edge))(functools.partial(stage_a, q))

    def inner_a(q, member):
        pl.when(both(both(valid[q // 2], member), inner))(functools.partial(stage_a, q))

    def edge_a(s, cond):
        @pl.when(both(edge, cond))
        def _():
            stage_a(2 * s)
            stage_a(2 * s + 1)

    @pl.when(first)
    def _():
        for k in range(steps):
            stage_d(k)

    @pl.when(first)
    def _():
        for j in range(heads):
            pair_copy(j).start()

    @pl.when(second)
    def _():
        for j in range(nc):
            pair_copy(j).start()

    c_folds(lambda copy: copy.start())
    edge_a(0, both(second, near[0]))

    @pl.when(second)
    def _():
        pair_all(heads).wait_recv()
        for j in range(heads):
            high, rem = split(oth[j])
            hi[pl.ds(j * size, size), :] = high
            lo[pl.ds(j * size, size), :] = rem
        for s in range(1, 1 + heads):
            compute(s)

    for s in range(1, slots):
        edge_a(s, both(second, valid[s]))

    def center_d(k):
        here = drin.at[(pl.ds(0, nd - 1),) + d_in(k)]
        remote(here, here, di_send, di_recv.at[k], partner).wait_recv()
        total = drin[(0,) + d_in(k)]
        for j in range(1, nd):
            total = total + drin[(j,) + d_in(k)]

        @pl.when(c == 0)
        def _():
            d_ref[d_at(0, k)] = total + a_ref[d_at(0, k)]

        @pl.when(c != 0)
        def _():
            ad_copy(k, 1).wait_recv()
            d_ref[d_at(c, k)] = total + adbuf[d_in(k)]

        for to in range(nd):
            if to not in (mid - 1, mid):
                pl.when(z == (mid - 1 if to < mid else mid))(dout_copy(k, to).start)
        spread_d(k)

    @pl.when(both(first, center))
    def _():
        for k in range(steps):
            center_d(k)

    def outer_d(k):
        @pl.when(both(first, jnp.logical_not(center)))
        def _():
            dout_copy(k, 0).wait_recv()
            spread_d(k)

    def gather_d(k):
        @pl.when(first)
        def _():
            here = d_rows(k, BLOCK - sub)
            remote(here, here, d_send, d_recv.at[k], partner).wait_recv()
            for m in range(1, nc):
                f_copy(k, m).start()

    def arrive_d(k):
        @pl.when(second)
        def _():
            here = d_rows(k, BLOCK)
            remote(here, here, f_send, f_recv.at[k], partner).wait_recv()

    own = both(both(first, c == 0), zb < heads)
    holds = c == (r * nc + zb) // wide
    spot = lax.rem(r * nc + zb, wide)

    def t_wait(j):
        remote(tin.at[j], tin.at[j], t_send.at[0, 0], t_recv.at[j], partner).wait_recv()

    def n_copy(i):
        return remote(psum, nbuf.at[r * nd + z], n_send, n_recv, device(i))

    def norm_part():
        for j in range(wide):
            pl.when(both(both(holds, jnp.logical_not(own)), spot == j))(functools.partial(t_wait, j))

        @pl.when(holds)
        def _():
            base = a_ref[rows(z * share, share), rows(spot * size, size)]
            block = jnp.where(own, d_ref[rows(lax.rem(z * share, PB), share), rows(lax.rem(r * nc + zb, heads) * size, size)], base + tin[spot])
            row = zo + lax.broadcasted_iota(jnp.int32, block.shape, 0)
            squares = jnp.where(row == lax.broadcasted_iota(jnp.int32, block.shape, 1), block * block, 0.0)
            acc = squares.reshape(share // 8, 8, size).sum(0)
            acc = sum(acc[:, i:i + LANES] for i in range(0, size, LANES))
            psum[...] = acc
            nbuf[r * nd + z] = acc

            @pl.loop(1, devices)
            def _(i):
                n_copy(i).start()

    members = (second, both(first, g >= heads), g < heads)
    events = []
    for member, lists_of, (arrive, step), (send, gap) in zip(members, (lists[nc:], lists[heads:nc], lists[:heads]), ARRIVALS, SENDS):
        for q in range(2 * max(map(len, lists_of))):
            needed = q // 2 <= heads
            for when, stage in enumerate((inner_a, stage_b, stage_c)):
                events.append((arrive + step * q + when * HOP, needed, when == 2, functools.partial(stage, q, member)))
            if send:
                events.append((send + gap * q, needed, True, functools.partial(edge_send, q, member)))
    for k in range(1, steps):
        events.append((OPEN + k, True, None, functools.partial(gather_d, k)))
    events.append((NORM, False, None, norm_part))
    events.sort(key=lambda e: e[0])

    def run(batch):
        for kind, cond in ((None, None), (False, inner), (True, jnp.logical_not(center))):
            todo = [e[3] for e in batch if e[2] is kind]

            def act():
                for event in todo:
                    event()

            if todo:
                act() if kind is None else pl.when(cond)(act)

    def advance(now):
        batch = []
        while events and events[0][0] <= now:
            batch.append(events.pop(0))
        run(batch)

    advance(EARLIEST)
    for k in range(steps):
        outer_d(k)

    @pl.when(first)
    def _():
        pair_all(nc).wait_recv()
        for j in range(nc):
            high, rem = split(oth[j])
            here = pl.ds(tile_rows + j * size, size)
            hi[here, :] = high
            lo[here, :] = rem
        for s in range(slots):
            pl.when(far[s])(functools.partial(compute, s))

    gather_d(0)
    arrive_d(0)
    clock = [OPEN]

    def tick():
        advance(clock[0])
        clock[0] += TICK

    for s in range(0, PB, BLOCK):
        e = s + BLOCK
        src = fact if s else d_ref
        inv = factor_block(work, src[s:e, s:e], tick)
        invs[s // BLOCK] = inv
        if s == 0:
            for k in range(1, steps):
                arrive_d(k)
        if e < PB:
            u = mm(inv, src[s:e, e:], ((1,), (0,)))
            fact[s:e, e:] = u
            for j in range(e, PB, BLOCK):
                fact[j:j + BLOCK, j:] = src[j:j + BLOCK, j:] - mm(u[:, j - e:j - e + BLOCK], u[:, j - e:], ((0,), (0,)))

    @pl.when(both(first, c < heads))
    def _():
        for i in range(1, steps):
            for j in range(i):
                d_ref[i * BLOCK:(i + 1) * BLOCK, j * BLOCK:(j + 1) * BLOCK] = (
                    d_ref[j * BLOCK:(j + 1) * BLOCK, i * BLOCK:(i + 1) * BLOCK].T)

    @pl.when(own)
    def _():
        for j in range(wide):
            tin[j] = d_ref[rows(z * share, share), j * size:(j + 1) * size]

    count = max([i + 1 for i, event in enumerate(events) if event[1]], default=0)
    run(events[:count])
    events = events[count:]

    @pl.when(g >= heads)
    def _():
        for j in range(heads):
            rest[:, j * size:(j + 1) * size] = fin[1 + j]

    @pl.when(g < heads)
    def _():
        rest[...] = d_ref[rows(c * size, size), :]

    for s in range(0, PB, BLOCK):
        e = s + BLOCK
        x = mm(rest[:, s:e], invs[s // BLOCK], ((1,), (1,)))
        x_ref[:, s:e] = x
        if e < PB:
            rest[:, e:] = rest[:, e:] - mm(x, fact[s:e, e:], ((1,), (0,)))

    run(events)

    @pl.when(jnp.logical_not(own))
    def _():
        for j in range(wide):
            pl.when(jnp.logical_not(both(holds, spot == j)))(functools.partial(t_wait, j))

    folded = jnp.logical_or(c == 0, both(first, zb < heads))
    for j in range(wide):
        at = pl.ds(j * size, size)
        out_ref[:, at] = jnp.where(folded, 0.0, a_ref[rows(z * share, share), at]) + tin[j]

    for count, cond in ((nr * nd - 1, holds), (nr * nd, jnp.logical_not(holds))):
        here = nbuf.at[pl.ds(0, count)]
        pl.when(cond)(remote(here, here, n_send, n_recv, partner).wait_recv)
    acc = jnp.zeros((8, LANES), F32)
    for j in range(nr * nd):
        acc = acc + nbuf[j]
    n_ref[...] = jnp.sqrt(jnp.sum(acc, keepdims=True) / (tile_cols * nc))

    def sent(ref, sem):
        remote(ref, ref, sem, n_recv, partner).wait_send()

    @pl.when(holds)
    def _():
        sent(spent, n_send)

    c_folds(lambda copy: copy.wait_send())

    @pl.when(first)
    def _():
        pair_all(heads).wait_send()
        sent(rows_of(nc * unit), f_send)
        sent(rows_of((nc - 1) * unit), d_send)

        @pl.when(center)
        def _():
            sent(rows_of(unit), di_send)
            for _ in range(mid - 1):
                sent(rows_of(unit), do_send)

            @pl.when(c == 0)
            def _():
                sent(rows_of((nc - 1) * unit), ad_send)

        @pl.when(jnp.logical_not(center))
        def _():
            sent(rows_of(2 * unit), di_send)

    @pl.when(second)
    def _():
        pair_all(nc).wait_send()

    def slots_sent(s, count, index):
        sent(part.at[pl.ds(s, count)], in_send.at[index])

        @pl.when(inner)
        def _():
            sent(fin.at[pl.ds(s, count)], out_send.at[index])

    slots_sent(0, base, 0)
    for s in range(base, slots):
        pl.when(valid[s])(functools.partial(slots_sent, s, 1, s - base + 1))

    for s in range(slots):
        for way, (cond, src, spot, to) in enumerate(routes(s)):
            @pl.when(both(cond, jnp.logical_not(here_is(to))))
            def _():
                remote(src, tin.at[spot], t_send.at[s, way], t_recv.at[spot], to).wait_send()


def local(sizes, a_tile, panels):
    nr, nc, nd = sizes
    tile_rows, tile_cols = a_tile.shape
    k_size = panels.shape[1]
    share, size = tile_rows // nd, tile_rows // nc
    heads, wide, steps, sub = PB // size, tile_cols // size, PB // BLOCK, BLOCK // nc
    lists = plan(nr, nc, heads)
    slots, base = max(map(len, lists)), min(map(len, lists))
    one = pltpu.SemaphoreType.DMA
    vmem = pl.BlockSpec(memory_space=pltpu.VMEM)
    buf = lambda *s: pltpu.VMEM(s, F32)
    dma = lambda *s: pltpu.SemaphoreType.DMA(s)
    trailing, new_panel, norm = pl.pallas_call(
        functools.partial(kernel, sizes, lists),
        out_shape=(buf(share, tile_cols), buf(size, PB), buf(1, 1)),
        in_specs=[pl.BlockSpec(memory_space=pl.ANY)] * 2,
        out_specs=(vmem,) * 3,
        scratch_shapes=[
            buf(tile_rows, tile_cols), buf(tile_rows, k_size),
            pltpu.VMEM((nr * tile_rows, k_size), BF16), pltpu.VMEM((nr * tile_rows, k_size), BF16),
            buf(nc, size, k_size), buf(slots, size, size), buf(2, slots, size, size), buf(slots, size, size),
            buf(slots, size, size), buf(wide, share, size),
            buf(nd, BLOCK, PB), buf(PB, PB), buf(BLOCK, PB), buf(2 * heads, size // 2, size),
            buf(8, LANES), buf(nr * nd, 8, LANES), buf(nr * nc * nd - 1, 8, LANES),
            buf(BLOCK, 2 * BLOCK), buf(steps, BLOCK, BLOCK), buf(PB, PB), buf(size, PB),
            dma(tile_rows // TILE + 1), one, one, one, dma(steps), dma(2, nc), dma(2 * heads),
            dma(slots - base + 1), dma(2, 2 * slots), dma(slots - base + 1), dma(2 * slots),
            one, dma(steps), one, dma(steps), one, dma(steps), one, dma(steps), dma(slots, 2), dma(wide), one, one,
        ],
        compiler_params=pltpu.CompilerParams(collective_id=0, has_side_effects=True, vmem_limit_bytes=62 << 20),
        name="trailing_update",
    )(a_tile, panels)
    return (trailing, new_panel, norm.reshape(1))


def solution(mesh):
    sizes = tuple(mesh.shape[axis] for axis in ("row", "col", "depth"))
    return jax.shard_map(
        functools.partial(local, sizes),
        mesh=mesh,
        in_specs=(P("row", "col"), P("row", "depth")),
        out_specs=(P(("row", "depth"), "col"), P(("row", "col"), None), P()),
        check_vma=False,
    )
```

```python
import functools

import jax
import jax.numpy as jnp
from jax import lax
from jax.experimental import pallas as pl
from jax.experimental.pallas import tpu as pltpu
from jax.sharding import PartitionSpec as P

PB = 512
BLOCK = 128
NB = 32
LANES = 128
TILE = 256
OPEN, TICK, HOP, NORM = 18.0, 1.0, 4.3, 42.0
ARRIVALS = ((13.5, 15.3, 18.0, 20.3, 22.6, 25.0, 27.5, 30.0, 32.5, 35.0), (24.5, 26.5, 29.0, 31.5, 33.8, 35.4, 37.0, 38.5))
EARLIEST = 16.5
SENDS = (16.5, 1.4)
MESH = pl.DeviceIdType.MESH
F32 = jnp.float32
BF16 = jnp.bfloat16


def split(value):
    high = value.astype(BF16)
    return high, (value - high.astype(F32)).astype(BF16)


def dot_t(left, right):
    return lax.dot_general(left, right, (((1,), (1,)), ((), ())), preferred_element_type=F32)


def product(left_hi, left_lo, right_hi, right_lo):
    return dot_t(left_hi, right_hi) + (dot_t(left_hi, right_lo) + dot_t(left_lo, right_hi))


def mm(a, b, dims):
    a_hi, a_lo = split(a)
    b_hi, b_lo = split(b)
    dot = lambda x, y: lax.dot_general(x, y, (dims, ((), ())), preferred_element_type=F32)
    return dot(a_hi, b_hi) + (dot(a_hi, b_lo) + dot(a_lo, b_hi))


def factor_block(work, block, advance):
    work[:, :BLOCK] = block
    diag = lax.broadcasted_iota(jnp.int32, (BLOCK, BLOCK), 0) == lax.broadcasted_iota(jnp.int32, (BLOCK, BLOCK), 1)
    work[:, BLOCK:] = jnp.where(diag, 1.0, 0.0)
    sub = lax.broadcasted_iota(jnp.int32, (NB, BLOCK), 0)
    for j in range(0, BLOCK, NB):
        left = work[j:j + NB, :BLOCK]
        right = work[j:j + NB, BLOCK:]
        advance()
        lanes = [jnp.broadcast_to(left[:, j + k:j + k + 1], (NB, BLOCK)) for k in range(NB)]
        for k in range(NB):
            inv = lax.rsqrt(lanes[k][k:k + 1])
            col = lanes[k] * inv
            for i in range(k + 1, NB):
                lanes[i] = lanes[i] - col * col[i:i + 1]
            row_l = left[k:k + 1] * inv
            row_r = right[k:k + 1] * inv
            below = jnp.where(sub > k, col, 0.0)
            left = jnp.where(sub == k, row_l, left - below * row_l)
            right = jnp.where(sub == k, row_r, right - below * row_r)
        work[j:j + NB, :BLOCK] = left
        work[j:j + NB, BLOCK:] = right
        if j + NB < BLOCK:
            both = jnp.concatenate([left, right], axis=1)
            work[j + NB:, :] = work[j + NB:, :] - mm(left[:, j + NB:], both, ((0,), (0,)))
    return work[:, BLOCK:]


def plan(nr, nc, heads, wide):
    lists = [[] for _ in range(nr * nc)]
    pairs = [(high, low) for low in range(heads, nr * nc) for high in range(low + 1, nr * nc)]
    for g in range(heads, nr * nc):
        lists[g] = [(g, g)] + [(g, j) for j in range(heads)]

    def far(g, pair):
        ends = [(x, y) for x, y in (pair, pair[::-1]) if x % nc in (0, nc - 1)]
        return sum((x // nc) * nc + y // wide != g for x, y in ends)

    late = {}
    for near in (True, False):
        for g in range(nc):
            found = [p for p in pairs if p[1] < nc and not far(g, p) and any(b % nc in (0, nc - 1) for b in p) == near]
            if g not in late and found:
                late[g] = found[0]
                pairs.remove(found[0])
    for high, low in pairs:
        able = [g for g in range(nr * nc) if g < nc or g // nc == low // nc]
        best = min(able, key=lambda g: (len(lists[g]) + (g in late), g not in (low, high), g))
        lists[best].append((high, low))
    for g, pair in late.items():
        lists[g].append(pair)
    base = min(map(len, lists))
    lists = [[pair + (3,) for pair in l] for l in lists]
    for g, l in enumerate(lists):
        for x, y, part in l[base:]:
            able = [h for h in range(nr * nc) if h % nc != g % nc and len(lists[h]) == base and (h < nc or h // nc == min(x, y) // nc)]
            if part == 3 and able:
                l[l.index((x, y, part))] = (x, y, 1)
                lists[able[-1]].append((x, y, 2))
    return lists


def kernel(sizes, lists, a_hbm, p_hbm, out_ref, x_ref, n_ref, *scratch):
    nr, nc, nd = sizes
    (a_ref, p_ref, hi, lo, oth, part, rin, fin, turned, tin, drin, d_ref, adbuf, acbuf, psum, nbuf, spent,
     work, invs, fact, rest,
     load, pair_send, pair_recv, ad_send, ad_recv, ac_send, ac_recv, in_send, in_recv, out_send, out_recv,
     di_send, di_recv, do_send, do_recv, d_send, d_recv, f_send, f_recv, t_send, t_recv, n_send, n_recv) = scratch
    tile_rows, tile_cols = a_ref.shape
    size = tile_rows // nc
    half = size // 2
    heads = PB // size
    wide = tile_cols // size
    share = tile_rows // nd
    sub = BLOCK // nc
    steps = PB // BLOCK
    slots, base = max(map(len, lists)), min(map(len, lists))
    unit = sub * (steps + 1) // 2
    devices = nr * nc * nd
    r, c, z = lax.axis_index("row"), lax.axis_index("col"), lax.axis_index("depth")
    g = r * nc + c
    mid = nd // 2
    low = z < mid
    center = jnp.logical_or(z == mid - 1, z == mid)
    edge = jnp.logical_or(z == 0, z == nd - 1)
    inner = jnp.logical_not(edge)
    side = jnp.where(center, 1, 0)
    inward = jnp.where(low, z + 1, z - 1)
    outward = jnp.where(low, z - 1, z + 1)
    zb = z * share // size
    zo = lax.rem(z * share, size)
    first, second = r == 0, r != 0
    partner = (1 - r, c, z)
    both = jnp.logical_and

    def pick(values):
        result = jnp.int32(values[0])
        for i, value in enumerate(values[1:], 1):
            result = jnp.where(g == i, value, result)
        return result

    xs = [pick([l[s][0] if s < len(l) else 0 for l in lists]) for s in range(slots)]
    ys = [pick([l[s][1] if s < len(l) else 0 for l in lists]) for s in range(slots)]
    counts = pick([len(l) for l in lists])
    masks = [pick([l[s][2] if s < len(l) else 0 for l in lists]) for s in range(slots)]
    valid = [s < counts for s in range(slots)]
    live = [both(valid[q // 2], masks[q // 2] != 2 - q % 2) for q in range(2 * slots)]
    near = [both(valid[s], both(xs[s] // nc == r, ys[s] // nc == r)) for s in range(slots)]
    far = [both(valid[s], jnp.logical_not(both(xs[s] // nc == r, ys[s] // nc == r))) for s in range(slots)]

    def remote(src, dst, send, recv, device):
        return pltpu.make_async_remote_copy(
            src_ref=src, dst_ref=dst, send_sem=send, recv_sem=recv, device_id=device, device_id_type=MESH)

    def rows(start, count):
        return pl.ds(pl.multiple_of(start, count), count)

    def p_load(t):
        at = pl.ds(t * TILE, TILE)
        return pltpu.make_async_copy(p_hbm.at[at, :], p_ref.at[at, :], load.at[t])

    a_load = pltpu.make_async_copy(a_hbm, a_ref, load.at[tile_rows // TILE])
    for t in range(tile_rows // TILE):
        p_load(t).start()
    a_load.start()

    barrier = pltpu.get_barrier_semaphore()
    me = g * nd + z

    def device(i):
        there = lax.rem(me + i, devices)
        return (there // (nc * nd), lax.rem(there // nd, nc), lax.rem(there, nd))

    @pl.loop(0, nd)
    def _(k):
        depth = lax.rem(z + k, nd)
        for i in range(nr * nc):
            to = (r if i < nc else 1 - r, lax.rem(c + i % nc, nc), depth)
            if i:
                pl.semaphore_signal(barrier, inc=1, device_id=to, device_id_type=MESH)
            else:
                @pl.when(k > 0)
                def _():
                    pl.semaphore_signal(barrier, inc=1, device_id=to, device_id_type=MESH)

    def split_own(t):
        p_load(t).wait()
        high, rem = split(p_ref[pl.ds(t * TILE, TILE), :])
        here = rows(r * tile_rows + t * TILE, TILE)
        hi[here, :] = high
        lo[here, :] = rem

    for t in range(PB // TILE):
        split_own(t)

    def compute(s):
        a, b = rows(xs[s] * size, size), rows(ys[s] * size, size)
        part[s] = -product(hi[a, :], lo[a, :], hi[b, :], lo[b, :])

    @pl.when(first)
    def _():
        at = [pl.ds(pl.multiple_of(k * BLOCK + c * sub, sub), sub) for k in range(steps)]
        left_hi = jnp.concatenate([hi[i, :] for i in at], axis=0)
        left_lo = jnp.concatenate([lo[i, :] for i in at], axis=0)
        drin[z] = -product(left_hi, left_lo, hi[:PB, :], lo[:PB, :])

    for t in range(PB // TILE, tile_rows // TILE):
        split_own(t)
    a_load.wait()
    for s in range(slots):
        pl.when(near[s])(functools.partial(compute, s))

    pl.semaphore_wait(barrier, devices - 1)

    def pair_copy(j):
        return remote(p_ref.at[rows(j * size, size), :], oth.at[j], pair_send, pair_recv.at[j], partner)

    def pair_all(count):
        return remote(oth.at[pl.ds(0, count)], oth.at[pl.ds(0, count)], pair_send, pair_recv.at[0], partner)

    def rows_of(count):
        return fact.at[pl.ds(0, count), :]

    def c_fold(q):
        return (mid - 1, mid, 0, nd - 1)[q % 4]

    def d_at(col, k):
        return (pl.ds(pl.multiple_of(k * BLOCK + col * sub, sub), sub), pl.ds(k * BLOCK, PB - k * BLOCK))

    def d_in(k):
        return (pl.ds(k * sub, sub), pl.ds(k * BLOCK, PB - k * BLOCK))

    def ad_copy(k, to):
        return remote(a_ref.at[d_at(to, k)], adbuf.at[d_in(k)], ad_send, ad_recv.at[k], (r, to, z))

    def ac_at(col, q):
        return (rows(col * size + q % 2 * half, half), pl.ds((q // 2 - 1) * size, size))

    def ac_copy(q, to):
        return remote(a_ref.at[ac_at(to, q)], acbuf.at[q - 2], ac_send.at[(q - 2) // 2, to], ac_recv.at[q - 2], (r, to, z))

    @pl.when(both(both(first, c == 0), center))
    def _():
        for k in range(steps):
            for to in range(1, nc):
                ad_copy(k, to).start()

    def c_folds(act):
        for q in range(2, 2 + 2 * heads):
            for to in range(1, nc):
                @pl.when(both(both(c == 0, z == c_fold(q)), r * nc + to >= heads))
                def _():
                    act(ac_copy(q, to))

    def din_copy(k, to):
        here = drin.at[(z,) + d_in(k)]
        return remote(here, here, di_send, di_recv.at[k], (r, c, to))

    def stage_d(k):
        for to in (mid - 1, mid):
            pl.when(z != to)(din_copy(k, to).start)

    def dout_copy(k, to):
        here = d_ref.at[d_at(c, k)]
        return remote(here, here, do_send, do_recv.at[k], (r, c, to))

    def d_copy(k, m):
        here = d_ref.at[d_at(c, k)]
        return remote(here, here, d_send, d_recv.at[k], (r, lax.rem(c + m, nc), z))

    def d_rows(k, count):
        return d_ref.at[pl.ds(k * BLOCK, count), pl.ds(k * BLOCK, PB - k * BLOCK)]

    def f_copy(k, m):
        there = d_ref.at[d_at(lax.rem(c - m + nc, nc), k)]
        return remote(there, there, f_send, f_recv.at[k], partner)

    def spread_d(k):
        for m in range(1, nc):
            d_copy(k, m).start()
        f_copy(k, 0).start()

    def chunk(q):
        return (q // 2, pl.ds(q % 2 * half, half), slice(None))

    def in_copy(q):
        return remote(part.at[chunk(q)], rin.at[(side,) + chunk(q)], in_send.at[max(0, q - 2 * base + 1)], in_recv.at[side, q], (r, c, inward))

    def in_wait(at, q):
        here = rin.at[(at,) + chunk(q)]
        remote(here, here, in_send.at[0], in_recv.at[at, q], (r, c, inward)).wait_recv()
        return here

    def out_copy(q):
        here = fin.at[chunk(q)]
        return remote(here, here, out_send.at[q], out_recv.at[q], (r, c, outward))

    def stage_a(q):
        @pl.when(inner)
        def _():
            part[chunk(q)] = part[chunk(q)] + in_wait(0, q)[...]

        if 0 < q // 2 <= heads:
            @pl.when(both(g >= heads, z == c_fold(q)))
            def _():
                @pl.when(c == 0)
                def _():
                    part[chunk(q)] = part[chunk(q)] + a_ref[ac_at(0, q)]

                @pl.when(c != 0)
                def _():
                    ac_copy(q, 1).wait_recv()
                    part[chunk(q)] = part[chunk(q)] + acbuf[q - 2]

        in_copy(q).start()

    def wanted(s, plane):
        last = plane * share // size
        reaches = lambda block: jnp.where(low, lax.rem(block, nc) <= last, lax.rem(block, nc) >= last)
        needed = jnp.logical_or(reaches(xs[s]), reaches(ys[s]))
        return jnp.logical_or(needed, g >= heads) if 0 < s <= heads else needed

    outgoing = [both(both(live[q], inner), wanted(q // 2, outward)) for q in range(2 * slots)]
    incoming = [both(both(live[q], jnp.logical_not(center)), wanted(q // 2, z)) for q in range(2 * slots)]

    def here_is(device):
        return both(device[0] == r, device[1] == c)

    def routes(q):
        s, h = q // 2, q % 2
        x, y = xs[s], ys[s]
        straight = (x // nc, y // wide, z)
        across = (y // nc, x // wide, z)
        found = []
        for e in range(1 if share == size else 2):
            cond = both(live[q], zb == lax.rem(x, nc))
            if share == size:
                cut, e = (pl.ds(h * half, half), slice(None)), h
                src = fin.at[(s,) + cut]
            else:
                cond = both(cond, zo // half == h)
                cut = (slice(None), pl.ds(e * half, half))
                src = fin.at[s, rows(zo, share), pl.ds(e * half, half)]
            found.append((cond, src, lax.rem(y, wide), cut, e, straight))
        cut = (slice(None), pl.ds(h * half, half))
        found.append((both(both(live[q], x != y), zb == lax.rem(y, nc)),
                      turned.at[s, rows(zo, share), pl.ds(h * half, half)], lax.rem(x, wide), cut, h, across))
        return found

    def route_copy(q, way):
        _, src, spot, cut, e, to = routes(q)[way]
        return remote(src, tin.at[(spot,) + cut], t_send.at[q, way], t_recv.at[spot, e], to)

    def deliver(q):
        found = routes(q)
        for way, (cond, src, spot, cut, e, to) in enumerate(found):
            @pl.when(cond)
            def _():
                if way == len(found) - 1:
                    turned[q // 2, :, pl.ds(q % 2 * half, half)] = fin[chunk(q)].T

                @pl.when(here_is(to))
                def _():
                    pltpu.make_async_copy(src, tin.at[(spot,) + cut], t_recv.at[spot, e]).start()

                pl.when(jnp.logical_not(here_is(to)))(route_copy(q, way).start)

    def stage_b(q, member):
        @pl.when(both(both(live[q], member), center))
        def _():
            fin[chunk(q)] = part[chunk(q)] + in_wait(1, q)[...]
            pl.when(outgoing[q])(out_copy(q).start)
            deliver(q)

    def stage_c(q, member):
        @pl.when(both(member, incoming[q]))
        def _():
            out_copy(q).wait_recv()
            pl.when(outgoing[q])(out_copy(q).start)
            deliver(q)

    def edge_send(q, member):
        pl.when(both(both(live[q], member), edge))(functools.partial(stage_a, q))

    def inner_a(q, member):
        pl.when(both(both(live[q], member), inner))(functools.partial(stage_a, q))

    def edge_a(s, cond):
        @pl.when(both(edge, cond))
        def _():
            for q in (2 * s, 2 * s + 1):
                if s < base:
                    stage_a(q)
                else:
                    pl.when(live[q])(functools.partial(stage_a, q))

    @pl.when(first)
    def _():
        for k in range(steps):
            stage_d(k)

    @pl.when(first)
    def _():
        for j in range(heads):
            pair_copy(j).start()

    @pl.when(second)
    def _():
        for j in range(nc):
            pair_copy(j).start()

    c_folds(lambda copy: copy.start())
    def split_pair(j, at):
        pair_copy(j).wait_recv()
        high, rem = split(oth[j])
        hi[pl.ds(at, size), :] = high
        lo[pl.ds(at, size), :] = rem

    @pl.when(second)
    def _():
        for j in range(heads):
            split_pair(j, j * size)
            compute(1 + j)
            if j == 0:
                edge_a(0, near[0])

    for s in range(1, slots):
        edge_a(s, both(second, valid[s]))

    def far_part(j):
        @pl.when(first)
        def _():
            split_pair(j, tile_rows + j * size)
            for s in range(slots):
                latest = jnp.maximum(xs[s], ys[s])
                pl.when(both(far[s], latest == nc + j))(functools.partial(compute, s))

    def center_d(k):
        here = drin.at[(pl.ds(0, nd - 1),) + d_in(k)]
        remote(here, here, di_send, di_recv.at[k], partner).wait_recv()
        total = drin[(0,) + d_in(k)]
        for j in range(1, nd):
            total = total + drin[(j,) + d_in(k)]

        @pl.when(c == 0)
        def _():
            d_ref[d_at(0, k)] = total + a_ref[d_at(0, k)]

        @pl.when(c != 0)
        def _():
            ad_copy(k, 1).wait_recv()
            d_ref[d_at(c, k)] = total + adbuf[d_in(k)]

        for to in range(nd):
            if to not in (mid - 1, mid):
                pl.when(z == (mid - 1 if to < mid else mid))(dout_copy(k, to).start)
        spread_d(k)

    @pl.when(both(first, center))
    def _():
        for k in range(steps):
            center_d(k)

    def outer_d(k):
        @pl.when(both(first, jnp.logical_not(center)))
        def _():
            dout_copy(k, 0).wait_recv()
            spread_d(k)

    def gather_d(k):
        @pl.when(first)
        def _():
            here = d_rows(k, BLOCK - sub)
            remote(here, here, d_send, d_recv.at[k], partner).wait_recv()
            for m in range(1, nc):
                f_copy(k, m).start()

    def arrive_d(k):
        @pl.when(second)
        def _():
            here = d_rows(k, BLOCK)
            remote(here, here, f_send, f_recv.at[k], partner).wait_recv()

    own = both(both(first, c == 0), zb < heads)
    holds = c == (r * nc + zb) // wide
    spot = lax.rem(r * nc + zb, wide)

    def t_wait(j):
        for h in range(2):
            at = pl.ds(h * half, half)
            here = tin.at[j, at, :] if share == size else tin.at[j, :, at]
            remote(here, here, n_send, t_recv.at[j, h], partner).wait_recv()

    def n_copy(i):
        return remote(psum, nbuf.at[r * nd + z], n_send, n_recv, device(i))

    def norm_part():
        for j in range(wide):
            pl.when(both(both(holds, jnp.logical_not(own)), spot == j))(functools.partial(t_wait, j))

        @pl.when(holds)
        def _():
            base = a_ref[rows(z * share, share), rows(spot * size, size)]
            block = jnp.where(own, d_ref[rows(lax.rem(z * share, PB), share), rows(lax.rem(r * nc + zb, heads) * size, size)], base + tin[spot])
            row = zo + lax.broadcasted_iota(jnp.int32, block.shape, 0)
            squares = jnp.where(row == lax.broadcasted_iota(jnp.int32, block.shape, 1), block * block, 0.0)
            acc = squares.reshape(share // 8, 8, size).sum(0)
            acc = sum(acc[:, i:i + LANES] for i in range(0, size, LANES))
            psum[...] = acc
            nbuf[r * nd + z] = acc

            @pl.loop(1, devices)
            def _(i):
                n_copy(i).start()

    members = (second, both(first, g >= heads), g < heads)
    events = []
    for group, (member, lists_of) in enumerate(zip(members, (lists[nc:], lists[heads:nc], lists[:heads]))):
        arrivals = ARRIVALS[min(group, 1)]
        for q in range(2 * max(map(len, lists_of))):
            needed = q // 2 <= heads
            arrive = arrivals[min(q, len(arrivals) - 1)]
            for when, stage in enumerate((inner_a, stage_b, stage_c)):
                events.append((arrive + when * HOP, needed, when == 2, functools.partial(stage, q, member)))
            if group:
                events.append((SENDS[0] + SENDS[1] * q, needed, True, functools.partial(edge_send, q, member)))
    for k in range(1, steps):
        events.append((OPEN + k, True, None, functools.partial(gather_d, k)))
    events.append((NORM, False, None, norm_part))
    events.sort(key=lambda e: e[0])

    def run(batch):
        for kind, cond in ((None, None), (False, inner), (True, jnp.logical_not(center))):
            todo = [e[3] for e in batch if e[2] is kind]

            def act():
                for event in todo:
                    event()

            if todo:
                act() if kind is None else pl.when(cond)(act)

    def advance(now):
        batch = []
        while events and events[0][0] <= now:
            batch.append(events.pop(0))
        run(batch)

    early = nc - 1
    for j in range(early):
        far_part(j)
    advance(EARLIEST)
    for k in range(steps):
        outer_d(k)

    for j in range(early, nc):
        far_part(j)

    gather_d(0)
    arrive_d(0)
    clock = [OPEN]

    def tick():
        advance(clock[0])
        clock[0] += TICK

    for s in range(0, PB, BLOCK):
        e = s + BLOCK
        src = fact if s else d_ref
        inv = factor_block(work, src[s:e, s:e], tick)
        invs[s // BLOCK] = inv
        if s == 0:
            for k in range(1, steps):
                arrive_d(k)
        if e < PB:
            u = mm(inv, src[s:e, e:], ((1,), (0,)))
            fact[s:e, e:] = u
            for j in range(e, PB, BLOCK):
                fact[j:j + BLOCK, j:] = src[j:j + BLOCK, j:] - mm(u[:, j - e:j - e + BLOCK], u[:, j - e:], ((0,), (0,)))

    @pl.when(both(first, c < heads))
    def _():
        for i in range(1, steps):
            for j in range(i):
                d_ref[i * BLOCK:(i + 1) * BLOCK, j * BLOCK:(j + 1) * BLOCK] = (
                    d_ref[j * BLOCK:(j + 1) * BLOCK, i * BLOCK:(i + 1) * BLOCK].T)

    @pl.when(own)
    def _():
        for j in range(wide):
            tin[j] = d_ref[rows(z * share, share), j * size:(j + 1) * size]

    count = max([i + 1 for i, event in enumerate(events) if event[1]], default=0)
    run(events[:count])
    events = events[count:]

    @pl.when(g >= heads)
    def _():
        for j in range(heads):
            rest[:, j * size:(j + 1) * size] = fin[1 + j]

    @pl.when(g < heads)
    def _():
        rest[...] = d_ref[rows(c * size, size), :]

    for s in range(0, PB, BLOCK):
        e = s + BLOCK
        x = mm(rest[:, s:e], invs[s // BLOCK], ((1,), (1,)))
        x_ref[:, s:e] = x
        if e < PB:
            rest[:, e:] = rest[:, e:] - mm(x, fact[s:e, e:], ((1,), (0,)))

    run(events)

    @pl.when(jnp.logical_not(own))
    def _():
        for j in range(wide):
            pl.when(jnp.logical_not(both(holds, spot == j)))(functools.partial(t_wait, j))

    folded = jnp.logical_or(c == 0, both(first, zb < heads))
    for j in range(wide):
        at = pl.ds(j * size, size)
        out_ref[:, at] = jnp.where(folded, 0.0, a_ref[rows(z * share, share), at]) + tin[j]

    for count, cond in ((nr * nd - 1, holds), (nr * nd, jnp.logical_not(holds))):
        here = nbuf.at[pl.ds(0, count)]
        pl.when(cond)(remote(here, here, n_send, n_recv, partner).wait_recv)
    acc = jnp.zeros((8, LANES), F32)
    for j in range(nr * nd):
        acc = acc + nbuf[j]
    n_ref[...] = jnp.sqrt(jnp.sum(acc, keepdims=True) / (tile_cols * nc))

    def sent(ref, sem):
        remote(ref, ref, sem, n_recv, partner).wait_send()

    @pl.when(holds)
    def _():
        sent(spent, n_send)

    c_folds(lambda copy: copy.wait_send())

    @pl.when(first)
    def _():
        pair_all(heads).wait_send()
        sent(rows_of(nc * unit), f_send)
        sent(rows_of((nc - 1) * unit), d_send)

        @pl.when(center)
        def _():
            sent(rows_of(unit), di_send)
            for _ in range(mid - 1):
                sent(rows_of(unit), do_send)

            @pl.when(c == 0)
            def _():
                sent(rows_of((nc - 1) * unit), ad_send)

        @pl.when(jnp.logical_not(center))
        def _():
            sent(rows_of(2 * unit), di_send)

    @pl.when(second)
    def _():
        pair_all(nc).wait_send()

    def slots_sent(s, count, index):
        sent(part.at[pl.ds(s, count)], in_send.at[index])

    slots_sent(0, base, 0)
    for q in range(2 * base, 2 * slots):
        pl.when(live[q])(functools.partial(sent, part.at[chunk(q)], in_send.at[q - 2 * base + 1]))
    for q in range(2 * slots):
        pl.when(outgoing[q])(functools.partial(sent, fin.at[chunk(q)], out_send.at[q]))
        for way, (cond, _, _, _, _, to) in enumerate(routes(q)):
            pl.when(both(cond, jnp.logical_not(here_is(to))))(route_copy(q, way).wait_send)


def local(sizes, a_tile, panels):
    nr, nc, nd = sizes
    tile_rows, tile_cols = a_tile.shape
    k_size = panels.shape[1]
    share, size = tile_rows // nd, tile_rows // nc
    heads, wide, steps, sub = PB // size, tile_cols // size, PB // BLOCK, BLOCK // nc
    lists = plan(nr, nc, heads, wide)
    slots, base = max(map(len, lists)), min(map(len, lists))
    one = pltpu.SemaphoreType.DMA
    vmem = pl.BlockSpec(memory_space=pltpu.VMEM)
    buf = lambda *s: pltpu.VMEM(s, F32)
    dma = lambda *s: pltpu.SemaphoreType.DMA(s)
    trailing, new_panel, norm = pl.pallas_call(
        functools.partial(kernel, sizes, lists),
        out_shape=(buf(share, tile_cols), buf(size, PB), buf(1, 1)),
        in_specs=[pl.BlockSpec(memory_space=pl.ANY)] * 2,
        out_specs=(vmem,) * 3,
        scratch_shapes=[
            buf(tile_rows, tile_cols), buf(tile_rows, k_size),
            pltpu.VMEM((nr * tile_rows, k_size), BF16), pltpu.VMEM((nr * tile_rows, k_size), BF16),
            buf(nc, size, k_size), buf(slots, size, size), buf(2, slots, size, size), buf(slots, size, size),
            buf(slots, size, size), buf(wide, share, size),
            buf(nd, BLOCK, PB), buf(PB, PB), buf(BLOCK, PB), buf(2 * heads, size // 2, size),
            buf(8, LANES), buf(nr * nd, 8, LANES), buf(nr * nc * nd - 1, 8, LANES),
            buf(BLOCK, 2 * BLOCK), buf(steps, BLOCK, BLOCK), buf(PB, PB), buf(size, PB),
            dma(tile_rows // TILE + 1), one, dma(nc), one, dma(steps), dma(2, nc), dma(2 * heads),
            dma(2 * (slots - base) + 1), dma(2, 2 * slots), dma(2 * slots), dma(2 * slots),
            one, dma(steps), one, dma(steps), one, dma(steps), one, dma(steps), dma(2 * slots, 2 if share == size else 3), dma(wide, 2), one, one,
        ],
        compiler_params=pltpu.CompilerParams(collective_id=0, has_side_effects=True, vmem_limit_bytes=62 << 20),
        name="trailing_update",
    )(a_tile, panels)
    return (trailing, new_panel, norm.reshape(1))


def solution(mesh):
    sizes = tuple(mesh.shape[axis] for axis in ("row", "col", "depth"))
    return jax.shard_map(
        functools.partial(local, sizes),
        mesh=mesh,
        in_specs=(P("row", "col"), P("row", "depth")),
        out_specs=(P(("row", "depth"), "col"), P(("row", "col"), None), P()),
        check_vma=False,
    )
```
